32 devices in a mesh: dp: 1 (over z), cp: 4 (over y), tp: 8 (over x, core).
Axes of the slice: x: 4, y: 4, z: 1, core: 2. Of those that a mesh axis runs over, the one named last changes fastest.
The devices are a block of a 4x4x8 slice.
Arguments:
- x: bfloat16 [8192, 2048], P(('dp', 'cp', 'tp'))
- g_attn: float32 [2048], replicated
- wq: bfloat16 [2048, 2048], P(None, 'tp')
- wk: bfloat16 [2048, 2048], P(None, 'tp')
- wv: bfloat16 [2048, 2048], P(None, 'tp')
- wo: bfloat16 [2048, 2048], P('tp')
- g_mlp: float32 [2048], replicated
- idx: int32 [8192, 6], P(('dp', 'cp', 'tp'))
- gates: float32 [8192, 6], P(('dp', 'cp', 'tp'))
- w1g: bfloat16 [64, 2048, 1408], P(('cp', 'tp'))
- w1u: bfloat16 [64, 2048, 1408], P(('cp', 'tp'))
- w2: bfloat16 [64, 1408, 2048], P(('cp', 'tp'))
- ws1g: bfloat16 [2048, 2816], P(None, 'tp')
- ws1u: bfloat16 [2048, 2816], P(None, 'tp')
- ws2: bfloat16 [2816, 2048], P('tp')
Outputs:
- output: bfloat16 [8192, 2048], P(('dp', 'cp', 'tp'))
All inputs are finite; a program needn't handle non-finite values.
Results may differ from the reference program's by a relative error of at most 0.0132251.
Values are sent between devices in bfloat16 or wider.
A program may use at most 768 MiB of HBM per device.

```python
import math
import jax
import jax.numpy as jnp
from jax import lax

D = 2048
HEADS = 16
KV_HEADS = 16
HEAD = 128
EXPERTS = 64
TOP = 6
FF = 1408
FF_SHARED = 2816
SEQ = 8192
CP = 4
TP = 8

DEVS = CP * TP
TOKENS_DEV = SEQ // DEVS
SLOTS = TOP * (2 * TOKENS_DEV // EXPERTS + 1)
SLOTS_E = DEVS * SLOTS
GROUP = HEADS // KV_HEADS
EPS = 1e-6
ROPE_BASE = 10000.0


def normal_weight(k, shape, fan_in, gain=1.0):
    return (jax.random.normal(k, shape, jnp.float32) * (gain * fan_in ** -0.5)).astype(jnp.bfloat16)


def draw_routing(route_key):
    key_heat, key_base, key_offs = jax.random.split(route_key, 3)
    repeat_count = 2 * TOKENS_DEV // EXPERTS + 1
    heat_bits = jax.random.bits(key_heat, (EXPERTS,), jnp.uint32)
    bit_shift = jnp.sum((heat_bits[:, None] >> jnp.arange(16, dtype=jnp.uint32)[None, :]) & jnp.uint32(1), axis=1)
    expert_weight = jnp.tile(jnp.left_shift(jnp.uint32(1), bit_shift), repeat_count)

    def pick_bases(dev_key):
        scores = (jax.random.bits(dev_key, (EXPERTS * repeat_count,), jnp.uint32) >> 17) * expert_weight
        return jnp.argsort(jnp.uint32(0x7FFFFFFF) - scores)[:TOKENS_DEV] % EXPERTS

    base_ids = jax.vmap(pick_bases)(jax.random.split(key_base, DEVS))
    offsets = jax.vmap(lambda dev_key: jax.random.permutation(dev_key, EXPERTS)[:TOP])(jax.random.split(key_offs, DEVS))
    routed = (base_ids[:, :, None] + offsets[:, None, :]) % EXPERTS
    return routed.reshape(SEQ, TOP).astype(jnp.int32)


def setup_inputs(seed: int = 0, part: int = 0) -> dict:
    key = jax.random.key(seed)
    kx, kr, kg = jax.random.split(jax.random.fold_in(key, part), 3)
    kw = jax.random.split(key, 12)
    wo_gain = (SEQ / (3.0 * (1.0 + math.log(SEQ)))) ** 0.5
    return {
        "x": jax.random.normal(kx, (SEQ, D), jnp.float32).astype(jnp.bfloat16),
        "g_attn": jax.random.uniform(kw[0], (D,), jnp.float32, 0.5, 1.5),
        "wq": normal_weight(kw[1], (D, HEADS * HEAD), D),
        "wk": normal_weight(kw[2], (D, KV_HEADS * HEAD), D),
        "wv": normal_weight(kw[3], (D, KV_HEADS * HEAD), D),
        "wo": normal_weight(kw[4], (HEADS * HEAD, D), HEADS * HEAD, wo_gain),
        "g_mlp": jax.random.uniform(kw[5], (D,), jnp.float32, 0.5, 1.5),
        "idx": draw_routing(kr),
        "gates": jax.random.uniform(kg, (SEQ, TOP), jnp.float32, 0.3, 0.7),
        "w1g": normal_weight(kw[6], (EXPERTS, D, FF), D),
        "w1u": normal_weight(kw[7], (EXPERTS, D, FF), D),
        "w2": normal_weight(kw[8], (EXPERTS, FF, D), FF, 1.5),
        "ws1g": normal_weight(kw[9], (D, FF_SHARED), D),
        "ws1u": normal_weight(kw[10], (D, FF_SHARED), D),
        "ws2": normal_weight(kw[11], (FF_SHARED, D), FF_SHARED, 1.5),
    }


def rms_norm(a, g):
    af = a.astype(jnp.float32)
    r = af * lax.rsqrt(jnp.mean(af * af, axis=-1, keepdims=True) + EPS)
    return (r * g).astype(jnp.bfloat16)


def rope(t, pos):
    half = HEAD // 2
    freq = ROPE_BASE ** (-jnp.arange(half, dtype=jnp.float32) / half)
    ang = pos.astype(jnp.float32)[:, None] * freq[None, :]
    c = jnp.cos(ang)[:, None, :]
    s = jnp.sin(ang)[:, None, :]
    t1 = t[..., :half]
    t2 = t[..., half:]
    return jnp.concatenate([t1 * c - t2 * s, t2 * c + t1 * s], axis=-1)


def layout_positions():
    i = jnp.arange(SEQ)
    half = SEQ // (2 * CP)
    r = i // (2 * half)
    w = i % (2 * half)
    return jnp.where(w < half, r * half + w, (2 * CP - 1 - r) * half + w - half)


def reference(x, g_attn, wq, wk, wv, wo, g_mlp, idx, gates, w1g, w1u, w2, ws1g, ws1u, ws2):
    f32 = jnp.float32
    bf16 = jnp.bfloat16
    pos = layout_positions()
    xn = rms_norm(x, g_attn)
    q = rope(jnp.dot(xn, wq, preferred_element_type=f32).reshape(SEQ, HEADS, HEAD), pos).astype(bf16)
    k = rope(jnp.dot(xn, wk, preferred_element_type=f32).reshape(SEQ, KV_HEADS, HEAD), pos).astype(bf16)
    v = jnp.dot(xn, wv, preferred_element_type=f32).astype(bf16).reshape(SEQ, KV_HEADS, HEAD)
    kh = jnp.repeat(k, GROUP, axis=1).transpose(1, 0, 2)
    vh = jnp.repeat(v, GROUP, axis=1).transpose(1, 0, 2)
    mask = pos[None, :] <= pos[:, None]

    def one_head(operands):
        qa, ka, va = operands
        s = jnp.dot(qa.astype(f32), ka.astype(f32).T) * HEAD ** -0.5
        p = jax.nn.softmax(jnp.where(mask, s, -1e30), axis=-1)
        return jnp.dot(p, va.astype(f32))

    o = lax.map(one_head, (q.transpose(1, 0, 2), kh, vh))
    o = o.transpose(1, 0, 2).reshape(SEQ, HEADS * HEAD).astype(bf16)
    h = (x.astype(f32) + jnp.dot(o, wo, preferred_element_type=f32)).astype(bf16)
    t = rms_norm(h, g_mlp)
    u = (jax.nn.silu(jnp.dot(t, ws1g, preferred_element_type=f32)) * jnp.dot(t, ws1u, preferred_element_type=f32)).astype(bf16)
    shared = jnp.dot(u, ws2, preferred_element_type=f32)
    flat_e = idx.reshape(-1)
    onehot = (flat_e[:, None] == jnp.arange(EXPERTS)[None, :]).astype(jnp.int32)
    rank = jnp.sum((jnp.cumsum(onehot, axis=0) - onehot) * onehot, axis=1)
    tok = jnp.arange(SEQ * TOP) // TOP
    tab = jnp.full((EXPERTS, SLOTS_E), SEQ, jnp.int32).at[flat_e, rank].set(tok)
    gtab = jnp.zeros((EXPERTS, SLOTS_E), f32).at[flat_e, rank].set(gates.reshape(-1))
    tpad = jnp.concatenate([t, jnp.zeros((1, D), t.dtype)], axis=0)

    def expert_step(acc, xs):
        a1, a2, a3, tb, gb = xs
        te = tpad[tb]
        act = (jax.nn.silu(jnp.dot(te, a1, preferred_element_type=f32)) * jnp.dot(te, a2, preferred_element_type=f32)).astype(bf16)
        z = jnp.dot(act, a3, preferred_element_type=f32).astype(bf16)
        return acc.at[tb].add(gb[:, None] * z.astype(f32)), None

    acc, _ = lax.scan(expert_step, jnp.zeros((SEQ + 1, D), f32), (w1g, w1u, w2, tab, gtab))
    return (h.astype(f32) + shared + acc[:SEQ]).astype(bf16)
```

```python
import functools

import jax
import jax.numpy as jnp
from jax import lax
from jax.experimental import pallas as pl
from jax.experimental.pallas import tpu as pltpu
from jax.sharding import PartitionSpec as P

HEAD = 128
EPS = 1e-6
ROPE_BASE = 10000.0
MESH = pl.DeviceIdType.MESH
VMEM_MAX = 66_500_000
f32 = jnp.float32
bf16 = jnp.bfloat16


def rms_norm(a, g):
    af = a.astype(f32)
    r = af * lax.rsqrt(jnp.mean(af * af, axis=-1, keepdims=True) + EPS)
    return (r * g).astype(bf16)


def layout_pos(i, ncp, seq):
    half = seq // (2 * ncp)
    r = i // (2 * half)
    w = i % (2 * half)
    return jnp.where(w < half, r * half + w, (2 * ncp - 1 - r) * half + w - half)


def qkv_kernel(x_ref, wq_ref, wk_ref, wv_ref, c_ref, s_ref, q_ref, kv_ref):
    xb = x_ref[...]
    c, s = c_ref[...], s_ref[...]
    width = wq_ref.shape[1]

    def put(w_ref, o_ref, at, turn):
        r = jnp.dot(xb, w_ref[...], preferred_element_type=f32)
        for hd in range(width // HEAD):
            a = r[:, hd * HEAD:(hd + 1) * HEAD]
            if turn:
                a = a * c + pltpu.roll(a, HEAD // 2, 1) * s
            o_ref[:, at + hd * HEAD:at + (hd + 1) * HEAD] = a.astype(bf16)

    put(wk_ref, kv_ref, 0, True)
    put(wv_ref, kv_ref, width, False)
    put(wq_ref, q_ref, 0, True)


def qkv(xg, wq, wk, wv, cos, sin):
    n, dm = xg.shape
    w = wq.shape[1]
    blk = 512
    whole = lambda a, b: pl.BlockSpec((a, b), lambda i: (0, 0))
    rowb = lambda b: pl.BlockSpec((blk, b), lambda i: (i, 0))
    return pl.pallas_call(
        qkv_kernel,
        grid=(n // blk,),
        in_specs=[rowb(dm), whole(dm, w), whole(dm, w), whole(dm, w), rowb(HEAD), rowb(HEAD)],
        out_specs=[rowb(w), rowb(2 * w)],
        out_shape=[jax.ShapeDtypeStruct((n, w), bf16), jax.ShapeDtypeStruct((n, 2 * w), bf16)],
        compiler_params=pltpu.CompilerParams(vmem_limit_bytes=48 * 2**20),
        cost_estimate=pl.CostEstimate(flops=6 * n * dm * w, bytes_accessed=2 * n * dm + 6 * dm * w + 6 * n * w, transcendentals=0),
    )(xg, wq, wk, wv, cos, sin)


def attn_kernel(ncp, piece, bq, bk, q_ref, k_ref, v_ref, o_ref, m_ref, l_ref, acc_ref):
    r = lax.axis_index("cp")
    qi = pl.program_id(1)
    per = piece // bq
    second = qi // per
    pq = jnp.where(second == 0, r, 2 * ncp - 1 - r)
    inner = qi % per
    scale = HEAD ** -0.5
    q = q_ref[...]
    m_ref[...] = jnp.full_like(m_ref, -1e30)
    l_ref[...] = jnp.zeros_like(l_ref)
    acc_ref[...] = jnp.zeros_like(acc_ref)

    def step(row, mask_off):
        row = pl.multiple_of(row, bk)
        k = k_ref[pl.ds(row, bk), :]
        v = v_ref[pl.ds(row, bk), :]
        s = lax.dot_general(q, k, (((1,), (1,)), ((), ())), preferred_element_type=f32)
        if mask_off is not None:
            qp = lax.broadcasted_iota(jnp.int32, s.shape, 0) + mask_off
            kp = lax.broadcasted_iota(jnp.int32, s.shape, 1)
            s = jnp.where(kp <= qp, s, -1e30)
        m_old = m_ref[:, :1]
        m_new = jnp.maximum(m_old, jnp.max(s, axis=1, keepdims=True))
        p = jnp.exp((s - m_new) * scale)
        a = jnp.exp((m_old - m_new) * scale)
        l_ref[...] = a * l_ref[...] + jnp.sum(p, axis=1, keepdims=True)
        acc_ref[...] = a * acc_ref[...] + jnp.dot(p.astype(bf16), v, preferred_element_type=f32)
        m_ref[...] = jnp.broadcast_to(m_new, m_ref.shape)

    def base_of(p):
        return jnp.where(p < ncp, p * (2 * piece), (2 * ncp - 1 - p) * (2 * piece) + piece)

    kper = piece // bk

    def full_piece(p, _):
        b = base_of(p)
        for j in range(kper):
            step(b + j * bk, None)
        return 0

    lax.fori_loop(0, pq, full_piece, 0)
    b = base_of(pq)
    first = inner * bq
    lax.fori_loop(0, first // bk, lambda j, _: (step(b + j * bk, None), 0)[1], 0)
    for j in range(max(bq // bk, 1)):
        at = first // bk * bk + j * bk
        step(b + at, first - at)
    o_ref[...] = (acc_ref[...] / l_ref[...]).astype(bf16)


def attention(q, kv, ncp):
    n, w = q.shape
    seq = kv.shape[0]
    heads = w // HEAD
    piece = n // 2
    bq, bk = 512, 512
    return pl.pallas_call(
        functools.partial(attn_kernel, ncp, piece, bq, bk),
        grid=(heads, n // bq),
        in_specs=[pl.BlockSpec((bq, HEAD), lambda h, i: (i, h)),
                  pl.BlockSpec((seq, HEAD), lambda h, i: (0, h)),
                  pl.BlockSpec((seq, HEAD), lambda h, i: (0, heads + h))],
        out_specs=pl.BlockSpec((bq, HEAD), lambda h, i: (i, h)),
        out_shape=jax.ShapeDtypeStruct((n, w), bf16),
        scratch_shapes=[pltpu.VMEM((bq, HEAD), f32)] * 3,
        compiler_params=pltpu.CompilerParams(vmem_limit_bytes=40 * 2**20),
        cost_estimate=pl.CostEstimate(flops=4 * n * seq * w, bytes_accessed=6 * seq * w, transcendentals=n * seq),
    )(q, kv, kv)


ORDER = [(0, 0), (1, 0), (3, 0), (0, 1), (0, 3), (2, 0), (0, 2), (1, 1),
         (1, 3), (3, 1), (3, 3), (2, 1), (2, 3), (1, 2), (3, 2), (2, 2)]
DIST = [0, 1, 2, 1]


def packed(values):
    return [sum(v << (2 * i) for i, v in enumerate(values[k:k + 8])) for k in (0, 8)]


DX, DY = packed([o[0] for o in ORDER]), packed([o[1] for o in ORDER])


def look(table, j):
    a, b = table
    return ((a + (j // 8) * (b - a)) >> (2 * (j % 8))) & 3


def gather_copies(rows):
    h, q = rows // 2, rows // 4
    out = []
    for flip in (False, True):
        base = h if flip else 0
        fw = (lambda a, b: (b, a)) if flip else (lambda a, b: (a, b))

        def add(blk, lo, n, step):
            out.append((fw(*blk), base + lo, n, fw(*step)))

        add((0, 0), 0, h, (1, 0))
        add((0, 0), 0, h, (3, 0))
        add((3, 0), 0, q, (1, 0))
        add((1, 0), q, q, (3, 0))
        for b in range(4):
            add((b, 0), 0, h, (0, 1))
            add((b, 0), 0, h, (0, 3))
            add((b, 3), 0, q, (0, 1))
            add((b, 1), q, q, (0, 3))
    return out


def dist(b):
    return DIST[b[0]] + DIST[b[1]]


def moe_kernel(nx, ny, cap, groups, t_ref, mc_ref, code_ref, gate_ref, w1g_ref, w1u_ref, w2_ref,
               acc_ref, tg_ref, rz_ref,
               vg, vu, vd, xin, act, zb, tb, zin,
               wsem, tsem, zsem, lsem, ag_s, ag_r, dd_s, dd_r, rt_s, rt_r):
    ntok, dm = t_ref.shape
    ff = w1g_ref.shape[2]
    y = lax.axis_index("cp")
    tp = lax.axis_index("tp")
    x, c = tp // 2, tp % 2
    nchip = nx * ny
    per = nchip // groups
    homes = 2 * per

    def dev(dx, dy, core):
        return {"cp": (y + dy) % ny, "tp": ((x + dx) % nx) * 2 + core}

    def flat(dx, dy, core):
        return ((y + dy) % ny) * (2 * nx) + ((x + dx) % nx) * 2 + core

    loads = [pltpu.make_async_copy(w1g_ref, vg, wsem.at[0]),
             pltpu.make_async_copy(w1u_ref, vu, wsem.at[1]),
             pltpu.make_async_copy(w2_ref, vd, wsem.at[2])]
    own = pltpu.make_async_copy(t_ref, tg_ref.at[flat(0, 0, c)], lsem.at[0])

    barrier = pltpu.get_barrier_semaphore()

    def greet(k, _):
        other = (y * 2 * nx + tp + k) % (2 * nchip)
        pl.semaphore_signal(barrier, inc=1, device_id={"cp": other // (2 * nx), "tp": other % (2 * nx)}, device_id_type=MESH)
        return 0

    lax.fori_loop(1, 2 * nchip, greet, 0)
    pl.semaphore_wait(barrier, 2 * nchip - 1)

    copies = gather_copies(ntok)

    def ici(k):
        blk, lo, n, step = copies[k]
        here = tg_ref.at[flat(blk[0], blk[1], c), pl.ds(lo, n), :]
        src = t_ref.at[pl.ds(lo, n), :] if blk == (0, 0) else here
        return pltpu.make_async_remote_copy(src_ref=src, dst_ref=here, send_sem=ag_s.at[k], recv_sem=ag_r.at[k],
                                            device_id=dev(step[0], step[1], c), device_id_type=MESH)

    def ici_in(k):
        blk, lo, n, step = copies[k]
        here = tg_ref.at[flat(blk[0] - step[0] + nx, blk[1] - step[1] + ny, c), pl.ds(lo, n), :]
        return pltpu.make_async_remote_copy(src_ref=here, dst_ref=here, send_sem=ag_s.at[k], recv_sem=ag_r.at[k],
                                            device_id=dev(nx - step[0], ny - step[1], c), device_id_type=MESH)

    def d2d(j, core):
        blk = ORDER[j]
        here = tg_ref.at[flat(blk[0], blk[1], core)]
        src = t_ref if (j == 0) else here
        return pltpu.make_async_remote_copy(src_ref=src, dst_ref=here, send_sem=dd_s.at[j], recv_sem=dd_r.at[j],
                                            device_id=dev(0, 0, 1 - c), device_id_type=MESH)

    def d2d_in(j):
        blk = ORDER[j]
        here = tg_ref.at[flat(blk[0], blk[1], 1 - c)]
        return pltpu.make_async_remote_copy(src_ref=here, dst_ref=here, send_sem=dd_s.at[j], recv_sem=dd_r.at[j],
                                            device_id=dev(0, 0, 1 - c), device_id_type=MESH)

    def round_(w):
        if w > 0:
            for k, cp in enumerate(copies):
                if dist(cp[0]) == w - 1:
                    ici_in(k).wait_recv()
        for k, cp in enumerate(copies):
            if dist(cp[0]) == w:
                ici(k).start()
        for j, b in enumerate(ORDER):
            if dist(b) == w:
                d2d(j, c).start()

    def siblings(w):
        for j, b in enumerate(ORDER):
            if dist(b) == w:
                d2d_in(j).wait_recv()

    round_(0)
    own.start()
    for l in loads:
        l.start()

    def back(j, s, slot):
        core = c if s == 0 else 1 - c
        return pltpu.make_async_remote_copy(src_ref=zb.at[slot], dst_ref=rz_ref.at[slot], send_sem=rt_s.at[slot],
                                            recv_sem=rt_r.at[slot],
                                            device_id=dev(look(DX, j), look(DY, j), core), device_id_type=MESH)

    def work(g, _):
        for w in range(1, 5):
            @pl.when(g == w - 1)
            def _():
                round_(w)
                if w == 1:
                    siblings(0)
                siblings(w)
                if w == 1:
                    own.wait()
                    for l in loads:
                        l.wait()

        def fetch(i):
            j = g * per + i // 2
            core = c if i % 2 == 0 else 1 - c
            d = flat(look(DX, j), look(DY, j), core)
            return d, pltpu.make_async_copy(tg_ref.at[d], tb.at[i % 2], tsem.at[i % 2])

        fetch(0)[1].start()
        for i in range(homes):
            d, cp = fetch(i)
            cp.wait()
            if i + 1 < homes:
                fetch(i + 1)[1].start()
            rows = lax.broadcasted_iota(jnp.int32, (2 * cap, ntok), 0)
            rank = jnp.where(rows < cap, mc_ref[0, pl.ds(d, 1), :], mc_ref[1, pl.ds(d, 1), :])
            sel = (rank == jnp.where(rows < cap, rows, rows - cap) + 1).astype(f32).astype(bf16)
            for n in range(0, dm, 512):
                got = jnp.dot(sel, tb[i % 2, :, n:n + 512], preferred_element_type=f32)
                xin[0, i * cap:(i + 1) * cap, n:n + 512] = got[:cap].astype(bf16)
                xin[1, i * cap:(i + 1) * cap, n:n + 512] = got[cap:].astype(bf16)

        for l in range(2):
            def up(at, n):
                a = jnp.dot(xin[l], vg[l, :, pl.ds(at, n)], preferred_element_type=f32)
                b = jnp.dot(xin[l], vu[l, :, pl.ds(at, n)], preferred_element_type=f32)
                act[:, pl.ds(at, n)] = (a * jax.nn.sigmoid(a) * b).astype(bf16)

            whole = ff // 256
            lax.fori_loop(0, whole, lambda n, _: (up(pl.multiple_of(n * 256, 256), 256), 0)[1], 0)
            if ff % 256:
                up(whole * 256, ff % 256)

            def down(n, _):
                at = pl.multiple_of(n * 256, 256)
                z = jnp.dot(act[...], vd[l, :, pl.ds(at, 256)], preferred_element_type=f32)
                for i in range(homes):
                    zb[g * homes + i, l * cap:(l + 1) * cap, pl.ds(at, 256)] = z[i * cap:(i + 1) * cap].astype(bf16)
                return 0

            lax.fori_loop(0, dm // 256, down, 0)

        for i in range(homes):
            j = g * per + i // 2
            if i == 0:
                @pl.when(g == 0)
                def _():
                    pltpu.make_async_copy(zb.at[0], rz_ref.at[0], lsem.at[1]).start()

                @pl.when(g > 0)
                def _():
                    back(j, 0, g * homes).start()
            else:
                back(j, i % 2, g * homes + i).start()
        return 0

    lax.fori_loop(0, groups, work, 0)

    acc_ref[...] = jnp.zeros_like(acc_ref)

    def arrived(j, s, slot):
        core = c if s == 0 else 1 - c
        return pltpu.make_async_remote_copy(src_ref=zb.at[slot], dst_ref=rz_ref.at[slot], send_sem=rt_s.at[slot],
                                            recv_sem=rt_r.at[slot],
                                            device_id=dev(nx - look(DX, j), ny - look(DY, j), core), device_id_type=MESH)

    def combine(j, _):
        @pl.when(j == 0)
        def _():
            pltpu.make_async_copy(zb.at[0], rz_ref.at[0], lsem.at[1]).wait()

        @pl.when(j > 0)
        def _():
            arrived(j, 0, 2 * j).wait_recv()

        arrived(j, 1, 2 * j + 1).wait_recv()
        pulls = [pltpu.make_async_copy(rz_ref.at[2 * j + s], zin.at[pl.ds(s * 2 * cap, 2 * cap), :], zsem.at[s]) for s in range(2)]
        for p in pulls:
            p.start()
        base = [flat(nx - look(DX, j), ny - look(DY, j), core) * (2 * cap) for core in (c, 1 - c)]
        lane = lax.broadcasted_iota(jnp.int32, (ntok, 4 * cap), 1)
        want = jnp.where(lane < 2 * cap, base[0] + lane, base[1] + lane - 2 * cap)
        g = jnp.zeros((ntok, 4 * cap), f32)
        for k in range(code_ref.shape[1]):
            g = g + jnp.where(code_ref[:, k:k + 1] == want, gate_ref[:, k:k + 1], 0.0)
        g1 = g.astype(bf16)
        rest = g - g1.astype(f32)
        g2 = rest.astype(bf16)
        g3 = (rest - g2.astype(f32)).astype(bf16)
        for p in pulls:
            p.wait()

        def col(n, _):
            at = pl.ds(pl.multiple_of(n * 512, 512), 512)
            z = zin[:, at]
            acc_ref[:, at] += (jnp.dot(g1, z, preferred_element_type=f32)
                               + (jnp.dot(g2, z, preferred_element_type=f32) + jnp.dot(g3, z, preferred_element_type=f32)))
            return 0

        lax.fori_loop(0, dm // 512, col, 0)
        return 0

    lax.fori_loop(0, nchip, combine, 0)

    for k in range(len(copies)):
        ici(k).wait_send()
    for j in range(nchip):
        d2d(j, c).wait_send()

    def drain(j, _):
        @pl.when(j > 0)
        def _():
            arrived(j, 0, 2 * j).wait_send()

        arrived(j, 1, 2 * j + 1).wait_send()
        return 0

    lax.fori_loop(0, nchip, drain, 0)


def moe(t, mc, code, gates, w1g, w1u, w2, nx, ny, cap):
    ntok, dm = t.shape
    nle, _, ff = w1g.shape
    ndev = 2 * nx * ny
    groups = 4
    rows = ndev // groups * cap
    any_ = pl.BlockSpec(memory_space=pl.ANY)
    vm = pl.BlockSpec(memory_space=pltpu.VMEM)
    ncopy = len(gather_copies(ntok))
    dma = pltpu.SemaphoreType.DMA
    return pl.pallas_call(
        functools.partial(moe_kernel, nx, ny, cap, groups),
        in_specs=[any_, vm, vm, vm, any_, any_, any_],
        out_specs=[vm, any_, any_],
        out_shape=[jax.ShapeDtypeStruct((ntok, dm), f32),
                   jax.ShapeDtypeStruct((ndev, ntok, dm), bf16),
                   jax.ShapeDtypeStruct((ndev, nle * cap, dm), bf16)],
        scratch_shapes=[pltpu.VMEM((nle, dm, ff), bf16), pltpu.VMEM((nle, dm, ff), bf16), pltpu.VMEM((nle, ff, dm), bf16),
                        pltpu.VMEM((nle, rows, dm), bf16), pltpu.VMEM((rows, ff), bf16),
                        pltpu.VMEM((ndev, nle * cap, dm), bf16), pltpu.VMEM((2, ntok, dm), bf16),
                        pltpu.VMEM((2 * nle * cap, dm), bf16),
                        dma((3,)), dma((2,)), dma((2,)), dma((2,)), dma((ncopy,)), dma((ncopy,)),
                        dma((nx * ny,)), dma((nx * ny,)), dma((ndev,)), dma((ndev,))],
        compiler_params=pltpu.CompilerParams(collective_id=0, has_side_effects=True, vmem_limit_bytes=VMEM_MAX),
        cost_estimate=pl.CostEstimate(flops=6 * ndev * nle * cap * dm * ff, bytes_accessed=10 * nle * dm * ff, transcendentals=0),
    )(t, mc, code, gates, w1g, w1u, w2)


def solution(mesh):
    ncp = mesh.shape["cp"]
    ntp = mesh.shape["tp"]
    ndev = ncp * ntp
    rows = P(("dp", "cp", "tp"), None)
    cols = P(None, "tp")
    wrows = P("tp", None)
    rep = P(None)
    exps = P(("cp", "tp"), None, None)

    def layer(x, g_attn, wq, wk, wv, wo, g_mlp, idx, gates, w1g, w1u, w2, ws1g, ws1u, ws2):
        r = lax.axis_index("cp")
        me = r * ntp + lax.axis_index("tp")
        ntok, dm = x.shape
        seq = ntok * ndev
        nloc = seq // ncp
        nle = w1g.shape[0]
        num_e = nle * ndev
        top = idx.shape[1]
        cap = -(-top * (2 * ntok // num_e + 1) // 8) * 8

        xg = lax.all_gather(rms_norm(x, g_attn), "tp", axis=0, tiled=True)
        idx_all = lax.all_gather(idx, ("cp", "tp"), axis=0, tiled=True)

        upto = (jnp.arange(ntok)[:, None] <= jnp.arange(ntok)[None, :]).astype(bf16)
        mine = me * nle + jnp.arange(nle)
        hit = jnp.any(idx_all[None] == mine[:, None, None], axis=-1).reshape(nle * ndev, ntok)
        mc = jnp.where(hit, jnp.dot(hit.astype(bf16), upto, preferred_element_type=f32), 0.0)
        mc = mc.astype(jnp.int32).reshape(nle, ndev, ntok)
        named = idx[:, :, None] == jnp.arange(num_e)[None, None, :]
        before = lax.dot_general(upto, jnp.any(named, axis=1).astype(bf16), (((0,), (0,)), ((), ())), preferred_element_type=f32) - 1.0
        rank = jnp.sum(jnp.where(named, before[:, None, :], 0.0), axis=-1).astype(jnp.int32)
        code = idx * cap + rank

        half = HEAD // 2
        pos = layout_pos(r * nloc + jnp.arange(nloc), ncp, seq)
        freq = ROPE_BASE ** (-jnp.arange(half, dtype=f32) / half)
        ang = pos.astype(f32)[:, None] * freq[None, :]
        cs, sn = jnp.cos(ang), jnp.sin(ang)
        q, kv = qkv(xg, wq, wk, wv, jnp.concatenate([cs, cs], 1), jnp.concatenate([-sn, sn], 1))
        kv_all = lax.all_gather(kv, "cp", axis=0, tiled=True)
        wo_all = lax.all_gather(wo, "tp", axis=0, tiled=True)
        ws2_all = lax.all_gather(ws2, "tp", axis=0, tiled=True)
        o = attention(q, kv_all, ncp)
        o = lax.all_to_all(o, "tp", 0, 1, tiled=True)
        attn = jnp.dot(o, wo_all, preferred_element_type=f32)
        h = (x.astype(f32) + attn).astype(bf16)
        t = rms_norm(h, g_mlp)

        routed, tg, _ = moe(t, mc, code, gates, w1g, w1u, w2, ntp // 2, ncp, cap)
        tl = lax.dynamic_slice_in_dim(tg, r * ntp, ntp, 0).reshape(nloc, dm)
        u = (jax.nn.silu(jnp.dot(tl, ws1g, preferred_element_type=f32)) * jnp.dot(tl, ws1u, preferred_element_type=f32)).astype(bf16)
        u = lax.all_to_all(u, "tp", 0, 1, tiled=True)
        shared = jnp.dot(u, ws2_all, preferred_element_type=f32)
        return (h.astype(f32) + shared + routed).astype(bf16)

    return jax.shard_map(layer, mesh=mesh,
                         in_specs=(rows, rep, cols, cols, cols, wrows, rep, rows, rows, exps, exps, exps, cols, cols, wrows),
                         out_specs=rows, check_vma=False)
```

```python
import functools

import jax
import jax.numpy as jnp
from jax import lax
from jax.experimental import pallas as pl
from jax.experimental.pallas import tpu as pltpu
from jax.sharding import PartitionSpec as P

HEAD = 128
EPS = 1e-6
ROPE_BASE = 10000.0
LOG2E = 1.4426950408889634
MESH = pl.DeviceIdType.MESH
DEPTH = 3
VMEM_MAX = 66_500_000
f32 = jnp.float32
bf16 = jnp.bfloat16


def rms_norm(a, g):
    af = a.astype(f32)
    r = af * lax.rsqrt(jnp.mean(af * af, axis=-1, keepdims=True) + EPS)
    return (r * g).astype(bf16)


def layout_pos(i, ncp, seq):
    half = seq // (2 * ncp)
    r = i // (2 * half)
    w = i % (2 * half)
    return jnp.where(w < half, r * half + w, (2 * ncp - 1 - r) * half + w - half)


def attn_kernel(x_ref, g_ref, wq_ref, wk_ref, wv_ref, c_ref, s_ref, wo_ref, ws2_ref, o_ref, wo_all, ws2_all,
                xg, q_s, kvb, m_s, l_s, acc_s, xs, xr, ds, dr, ys, yr, gs, gr, gd, ge, gl):
    ntok, dm = x_ref.shape
    w = wq_ref.shape[1]
    heads = w // HEAD
    r = lax.axis_index("cp")
    tp = lax.axis_index("tp")
    ncp, nch = kvb.shape[0], kvb.shape[1]
    nx = nch // 2
    x, c = tp // 2, tp % 2
    cexp = HEAD ** -0.5 * LOG2E

    def block(dx, core):
        return ((x + dx) % nx) * 2 + core

    def to_x(dx):
        return {"tp": block(dx, c)}

    def to_y(dy):
        return {"cp": (r + dy) % ncp}

    a = x_ref[...].astype(f32)
    n = a * lax.rsqrt(jnp.mean(a * a, axis=-1, keepdims=True) + EPS)
    xg[tp] = (n * g_ref[...]).astype(bf16)

    barrier = pltpu.get_barrier_semaphore()
    for d in (to_x(1), to_x(nx - 1), to_y(1), to_y(ncp - 1), {"tp": block(0, 1 - c)}):
        pl.semaphore_signal(barrier, inc=1, device_id=d, device_id_type=MESH)
    pl.semaphore_wait(barrier, 5)

    half = ntok // 2

    def xcopy(k, incoming=False):
        step = 1 if k in (0, 2) else nx - 1
        src = 0 if k < 2 else nx - step
        lo, num = ((0, ntok), (0, ntok), (0, half), (half, half))[k]
        at = (src - step) % nx if incoming else src
        ref = xg.at[block(at, c), pl.ds(lo, num), :]
        return pltpu.make_async_remote_copy(src_ref=ref, dst_ref=ref, send_sem=xs.at[k], recv_sem=xr.at[k],
                                            device_id=to_x(nx - step if incoming else step), device_id_type=MESH)

    def sib(dx, incoming=False):
        ref = xg.at[block(dx, 1 - c if incoming else c)]
        return pltpu.make_async_remote_copy(src_ref=ref, dst_ref=ref, send_sem=ds.at[dx], recv_sem=dr.at[dx],
                                            device_id={"tp": block(0, 1 - c)}, device_id_type=MESH)

    def ycopy(dx, s, k, incoming=False):
        step = 1 if k in (0, 2) else ncp - 1
        src = 0 if k < 2 else ncp - step
        rows = kvb.shape[2]
        lo, num = ((0, rows), (0, rows), (0, rows // 2), (rows // 2, rows // 2))[k]
        at = (src - step) % ncp if incoming else src
        b = block(dx, c if s == 0 else 1 - c)
        ref = kvb.at[(r + at) % ncp, b, pl.ds(lo, num), :]
        sem = (dx * 2 + s) * 4 + k
        return pltpu.make_async_remote_copy(src_ref=ref, dst_ref=ref, send_sem=ys.at[sem], recv_sem=yr.at[sem],
                                            device_id=to_y(ncp - step if incoming else step), device_id_type=MESH)

    shards = ((wo_ref, wo_all), (ws2_ref, ws2_all))

    def wcopy(a, k, incoming=False):
        own, full = shards[a]
        num = own.shape[0]
        step = 1 if k in (0, 2) else nx - 1
        src = 0 if k < 2 else nx - step
        lo, num = ((0, num), (0, num), (0, num // 2), (num // 2, num // 2))[k]
        at = (src - step) % nx if incoming else src
        ref = full.at[block(at, c), pl.ds(lo, num), :]
        return pltpu.make_async_remote_copy(src_ref=own if k < 2 and not incoming else ref, dst_ref=ref,
                                            send_sem=gs.at[a, k], recv_sem=gr.at[a, k],
                                            device_id=to_x(nx - step if incoming else step), device_id_type=MESH)

    def wsib(a, dx, incoming=False):
        own, full = shards[a]
        ref = full.at[block(dx, 1 - c if incoming else c)]
        return pltpu.make_async_remote_copy(src_ref=own if dx == 0 and not incoming else ref, dst_ref=ref,
                                            send_sem=gd.at[a, dx], recv_sem=ge.at[a, dx],
                                            device_id={"tp": block(0, 1 - c)}, device_id_type=MESH)

    def wown(a):
        return pltpu.make_async_copy(shards[a][0], shards[a][1].at[tp], gl.at[a])

    def wstart(a):
        wcopy(a, 0).start()
        wcopy(a, 1).start()
        wsib(a, 0).start()
        wown(a).start()

    def wpass(a):
        wcopy(a, 0, True).wait_recv()
        wcopy(a, 2).start()
        wcopy(a, 1, True).wait_recv()
        wcopy(a, 3).start()
        wsib(a, nx - 1).start()
        wsib(a, 1).start()

    def wlast(a):
        wcopy(a, 2, True).wait_recv()
        wcopy(a, 3, True).wait_recv()
        wsib(a, 2).start()

    def wend(a):
        wown(a).wait()
        for k in range(4):
            wcopy(a, k).wait_send()
        for dx in range(nx):
            wsib(a, dx, True).wait_recv()
            wsib(a, dx).wait_send()

    def qkv(dx, s):
        b = block(dx, c if s == 0 else 1 - c)
        at = pl.ds(pl.multiple_of(b * ntok, ntok), ntok)
        xb = xg[b]
        cs, sn = c_ref[at, :], s_ref[at, :]

        def turned(t):
            return (t * cs + pltpu.roll(t, HEAD // 2, 1) * sn)

        k = jnp.dot(xb, wk_ref[...], preferred_element_type=f32)
        for h in range(heads):
            kvb[r, b, h * HEAD:(h + 1) * HEAD, :] = turned(k[:, h * HEAD:(h + 1) * HEAD]).T.astype(bf16)
        kvb[r, b, w:, :] = jnp.dot(xb, wv_ref[...], preferred_element_type=f32).astype(bf16)
        q = jnp.dot(xb, wq_ref[...], preferred_element_type=f32)
        for h in range(heads):
            q_s[at, h * HEAD:(h + 1) * HEAD] = turned(q[:, h * HEAD:(h + 1) * HEAD]).astype(bf16)
        ycopy(dx, s, 0).start()
        ycopy(dx, s, 1).start()

    def pass_on(dx, s):
        for k in (0, 1):
            ycopy(dx, s, k, True).wait_recv()
        for k in (2, 3):
            ycopy(dx, s, k).start()

    xcopy(0).start()
    xcopy(1).start()
    sib(0).start()
    m_s[...] = jnp.full_like(m_s, -1e30)
    l_s[...] = jnp.zeros_like(l_s)
    acc_s[...] = jnp.zeros_like(acc_s)
    qkv(0, 0)
    sib(0, True).wait_recv()
    qkv(0, 1)
    xcopy(0, True).wait_recv()
    xcopy(2).start()
    sib(nx - 1).start()
    xcopy(1, True).wait_recv()
    xcopy(3).start()
    sib(1).start()
    qkv(nx - 1, 0)
    qkv(1, 0)
    for dx in (nx - 1, 1):
        sib(dx, True).wait_recv()
        qkv(dx, 1)
    for s in (0, 1):
        pass_on(0, s)
    wstart(0)
    wstart(1)
    xcopy(2, True).wait_recv()
    xcopy(3, True).wait_recv()
    sib(2).start()
    qkv(2, 0)
    sib(2, True).wait_recv()
    qkv(2, 1)

    def attend(h, qb, rank, kb, chunks, diag):
        rows = pl.ds(pl.multiple_of(qb * ntok, ntok), ntok)
        cols = slice(h * HEAD, (h + 1) * HEAD)
        q = q_s[rows, cols]
        sc = []
        for j in range(chunks):
            t = jnp.dot(q, kvb[rank, kb + j, cols, :], preferred_element_type=f32)
            if diag and j == chunks - 1:
                t = jnp.where(lax.broadcasted_iota(jnp.int32, t.shape, 1) <= lax.broadcasted_iota(jnp.int32, t.shape, 0), t, -1e30)
            sc.append(t)
        m_old = m_s[h, rows, :]
        top = sc[0]
        for t in sc[1:]:
            top = jnp.maximum(top, t)
        m_new = jnp.maximum(m_old, jnp.max(top, axis=1, keepdims=True))
        alpha = jnp.exp2((m_old - m_new) * cexp)
        ps = [jnp.exp2((t - m_new[:, :1]) * cexp) for t in sc]
        tot = ps[0]
        for p in ps[1:]:
            tot = tot + p
        pv = None
        for j, p in enumerate(ps):
            t = jnp.dot(p.astype(bf16), kvb[rank, kb + j, w:, cols], preferred_element_type=f32)
            pv = t if pv is None else pv + t
        l_s[h, rows, :] = alpha * l_s[h, rows, :] + jnp.sum(tot, axis=1, keepdims=True)
        acc_s[h, rows, :] = alpha * acc_s[h, rows, :] + pv
        m_s[h, rows, :] = m_new

    per = nch // 2

    def full(rank, qbase, kb):
        def go(i, _):
            for h in range(heads):
                attend(h, qbase + i, rank, kb, per, False)
            return 0

        lax.fori_loop(0, per, go, 0)

    def own_diag(second, _):
        base = second * per
        for i in range(per):
            for h in range(heads):
                attend(h, base + i, r, base, i + 1, True)
        return 0

    lax.fori_loop(0, 2, own_diag, 0)
    for dx in (nx - 1, 1):
        for s in (0, 1):
            pass_on(dx, s)
    full(r, per, 0)
    for s in (0, 1):
        pass_on(2, s)
    wpass(0)

    def other(dy):
        rank = (r + dy) % ncp
        low = jnp.where(rank < r, 0, per)
        full(rank, per, 0)
        full(rank, low, low)

    other(1)
    wlast(0)
    other(ncp - 1)
    wpass(1)
    for dx in range(nx):
        for s in (0, 1):
            for k in (2, 3):
                ycopy(dx, s, k, True).wait_recv()
    other(2)
    wlast(1)
    for h in range(heads):
        o_ref[:, h * HEAD:(h + 1) * HEAD] = (acc_s[h] / l_s[h]).astype(bf16)

    wend(0)
    wend(1)
    for k in range(4):
        xcopy(k).wait_send()
    for dx in range(nx):
        sib(dx).wait_send()
        for s in (0, 1):
            for k in range(4):
                ycopy(dx, s, k).wait_send()


def attention(x, g, wq, wk, wv, cos, sin, wo, ws2, ncp, ntp):
    ntok, dm = x.shape
    w = wq.shape[1]
    heads = w // HEAD
    n = ntok * ntp
    vm = pl.BlockSpec(memory_space=pltpu.VMEM)
    any_ = pl.BlockSpec(memory_space=pl.ANY)
    dma = pltpu.SemaphoreType.DMA
    return pl.pallas_call(
        attn_kernel,
        in_specs=[vm] * 7 + [any_] * 2,
        out_specs=[vm, any_, any_],
        out_shape=[jax.ShapeDtypeStruct((n, w), bf16), jax.ShapeDtypeStruct((ntp,) + wo.shape, bf16),
                   jax.ShapeDtypeStruct((ntp,) + ws2.shape, bf16)],
        scratch_shapes=[pltpu.VMEM((ntp, ntok, dm), bf16), pltpu.VMEM((n, w), bf16), pltpu.VMEM((ncp, ntp, 2 * w, ntok), bf16),
                        pltpu.VMEM((heads, n, HEAD), f32), pltpu.VMEM((heads, n, HEAD), f32), pltpu.VMEM((heads, n, HEAD), f32),
                        dma((4,)), dma((4,)), dma((ntp // 2,)), dma((ntp // 2,)), dma((4 * ntp,)), dma((4 * ntp,)),
                        dma((2, 4)), dma((2, 4)), dma((2, ntp // 2)), dma((2, ntp // 2)), dma((2,))],
        compiler_params=pltpu.CompilerParams(collective_id=1, has_side_effects=True, vmem_limit_bytes=60 * 2**20),
        cost_estimate=pl.CostEstimate(flops=6 * n * dm * w + 2 * n * n * ncp * w, bytes_accessed=16 * n * dm, transcendentals=0),
    )(x, g.reshape(1, dm), wq, wk, wv, cos, sin, wo, ws2)


ORDER = [(0, 0), (1, 0), (3, 0), (0, 1), (0, 3), (2, 0), (0, 2), (1, 1),
         (1, 3), (3, 1), (3, 3), (2, 1), (2, 3), (1, 2), (3, 2), (2, 2)]
DIST = [0, 1, 2, 1]


def packed(values):
    return [sum(v << (2 * i) for i, v in enumerate(values[k:k + 8])) for k in (0, 8)]


DX, DY = packed([o[0] for o in ORDER]), packed([o[1] for o in ORDER])


def look(table, j):
    a, b = table
    return ((a + (j // 8) * (b - a)) >> (2 * (j % 8))) & 3


def gather_copies(rows):
    h, q = rows // 2, rows // 4
    out = []
    for flip in (False, True):
        base = h if flip else 0
        fw = (lambda a, b: (b, a)) if flip else (lambda a, b: (a, b))

        def add(rank, blk, lo, n, step):
            out.append((rank, fw(*blk), base + lo, n, fw(*step)))

        add(0, (0, 0), 0, h, (1, 0))
        add(0, (0, 0), 0, h, (3, 0))
        add(1, (3, 0), 0, q, (1, 0))
        add(1, (1, 0), q, q, (3, 0))
        for b in (3, 1, 0, 2):
            add(2, (b, 0), 0, h, (0, 1))
            add(2, (b, 0), 0, h, (0, 3))
            add(3, (b, 3), 0, q, (0, 1))
            add(3, (b, 1), q, q, (0, 3))
    out.sort(key=lambda t: t[0])
    return [t[1:] for t in out]


def send_order():
    q = {d: [(d, e, s) for e in es for s in (0, 1) if (d, e, s) != (0, 0, 0)]
         for d, es in {0: (1, 3, 2, 0), 1: (1, 3, 2, 0), 3: (3, 1, 0, 2), 2: (0, 2, 1, 3)}.items()}
    out = []
    while any(q.values()):
        for d in (1, 3, 1, 3, 2, 0, 2, 0):
            if q[d]:
                dx, dy, s = q[d].pop(0)
                out.append((ORDER.index((dx, dy)), s))
    return out


def dist(b):
    return DIST[b[0]] + DIST[b[1]]


def moe_kernel(nx, ny, cap, groups, t_ref, idx_ref, code_ref, gate_ref, w1g_ref, w1u_ref, w2_ref,
               ws1_ref, ws2_ref, acc_ref, tg_ref, rz_ref, ru_ref,
               vg, vu, vd, xin, act, zb, tb, zin, ia, mc_ref,
               wsem, tsem, zsem, lsem, ag_s, ag_r, dd_s, dd_r, rt_s, rt_r, ix_s, ix_r,
               us_s, us_r, ssem):
    ntok, dm = t_ref.shape
    ff = w1g_ref.shape[2]
    y = lax.axis_index("cp")
    tp = lax.axis_index("tp")
    x, c = tp // 2, tp % 2
    nchip = nx * ny
    per = nchip // groups
    homes = 2 * per

    def dev(dx, dy, core):
        return {"cp": (y + dy) % ny, "tp": ((x + dx) % nx) * 2 + core}

    def flat(dx, dy, core):
        return ((y + dy) % ny) * (2 * nx) + ((x + dx) % nx) * 2 + core

    def weights(l):
        return [pltpu.make_async_copy(a.at[l, pl.ds(k * (a.shape[1] // 4), a.shape[1] // 4), :],
                                      b.at[l, pl.ds(k * (a.shape[1] // 4), a.shape[1] // 4), :], wsem.at[l, n, k])
                for n, (a, b) in enumerate(((w1g_ref, vg), (w1u_ref, vu), (w2_ref, vd))) for k in range(4)]

    own = pltpu.make_async_copy(t_ref, tg_ref.at[flat(0, 0, c)], lsem.at[0])

    ia[flat(0, 0, c)] = idx_ref[...]
    barrier = pltpu.get_barrier_semaphore()

    def greet(k, _):
        other = (y * 2 * nx + tp + k) % (2 * nchip)
        pl.semaphore_signal(barrier, inc=1, device_id={"cp": other // (2 * nx), "tp": other % (2 * nx)}, device_id_type=MESH)
        return 0

    lax.fori_loop(1, 2 * nchip, greet, 0)
    pl.semaphore_wait(barrier, 2 * nchip - 1)

    copies = gather_copies(ntok)

    def ici(k):
        blk, lo, n, step = copies[k]
        here = tg_ref.at[flat(blk[0], blk[1], c), pl.ds(lo, n), :]
        src = t_ref.at[pl.ds(lo, n), :] if blk == (0, 0) else here
        return pltpu.make_async_remote_copy(src_ref=src, dst_ref=here, send_sem=ag_s.at[k], recv_sem=ag_r.at[k],
                                            device_id=dev(step[0], step[1], c), device_id_type=MESH)

    def ici_in(k):
        blk, lo, n, step = copies[k]
        here = tg_ref.at[flat(blk[0] - step[0] + nx, blk[1] - step[1] + ny, c), pl.ds(lo, n), :]
        return pltpu.make_async_remote_copy(src_ref=here, dst_ref=here, send_sem=ag_s.at[k], recv_sem=ag_r.at[k],
                                            device_id=dev(nx - step[0], ny - step[1], c), device_id_type=MESH)

    def d2d(j, core):
        blk = ORDER[j]
        here = tg_ref.at[flat(blk[0], blk[1], core)]
        src = t_ref if (j == 0) else here
        return pltpu.make_async_remote_copy(src_ref=src, dst_ref=here, send_sem=dd_s.at[j], recv_sem=dd_r.at[j],
                                            device_id=dev(0, 0, 1 - c), device_id_type=MESH)

    def d2d_in(j):
        blk = ORDER[j]
        here = tg_ref.at[flat(blk[0], blk[1], 1 - c)]
        return pltpu.make_async_remote_copy(src_ref=here, dst_ref=here, send_sem=dd_s.at[j], recv_sem=dd_r.at[j],
                                            device_id=dev(0, 0, 1 - c), device_id_type=MESH)

    def round_(w):
        h = ntok // 2
        if w == 0:
            for k, cp in enumerate(copies):
                if cp[0] == (0, 0):
                    ici(k).start()
            d2d(0, c).start()
            return
        left = {}
        into = [(k, ((cp[0][0] - cp[3][0]) % nx, (cp[0][1] - cp[3][1]) % ny), cp) for k, cp in enumerate(copies) if dist(cp[0]) == w - 1]
        for k, blk, cp in into:
            part = (blk, cp[1] // h)
            left[part] = left.get(part, 0) + cp[2]
        done = {}
        for k, blk, cp in into:
            ici_in(k).wait_recv()
            part = (blk, cp[1] // h)
            left[part] -= cp[2]
            if left[part] == 0:
                for n, out in enumerate(copies):
                    if out[0] == blk and out[1] // h == part[1]:
                        ici(n).start()
                done[blk] = done.get(blk, 0) + 1
                if done[blk] == 2:
                    d2d(ORDER.index(blk), c).start()

    def siblings(w):
        for j, b in enumerate(ORDER):
            if dist(b) == w:
                d2d_in(j).wait_recv()

    def choices(j, s, incoming=False):
        core = c if s == 0 else 1 - c
        dx, dy = look(DX, j), look(DY, j)
        ref = ia.at[flat(nx - dx, ny - dy, core) if incoming else flat(0, 0, c)]
        return pltpu.make_async_remote_copy(src_ref=ref, dst_ref=ref, send_sem=ix_s.at[2 * j + s], recv_sem=ix_r.at[2 * j + s],
                                            device_id=dev(nx - dx, ny - dy, core) if incoming else dev(dx, dy, core),
                                            device_id_type=MESH)

    def each_other(do):
        def go(j, _):
            @pl.when(j > 0)
            def _():
                do(j, 0)

            do(j, 1)
            return 0

        lax.fori_loop(0, nchip, go, 0)

    each_other(lambda j, s: choices(j, s).start())
    round_(0)
    own.start()
    for l in range(2):
        for p in weights(l):
            p.start()

    def back(j, s, slot):
        core = c if s == 0 else 1 - c
        return pltpu.make_async_remote_copy(src_ref=zb.at[slot], dst_ref=rz_ref.at[slot], send_sem=rt_s.at[slot],
                                            recv_sem=rt_r.at[slot],
                                            device_id=dev(look(DX, j), look(DY, j), core), device_id_type=MESH)

    wide = ws1_ref.shape[1] // 2
    deep = ws2_ref.shape[1]

    def ublock(i):
        return xin.at[i // nx, pl.ds(0, ntok), pl.ds((i % nx) * wide, wide)]

    def ucopy(i, incoming=False):
        dx, core = i // 2, c if i % 2 == 0 else 1 - c
        return pltpu.make_async_remote_copy(src_ref=ublock(i), dst_ref=ru_ref.at[i], send_sem=us_s.at[i], recv_sem=us_r.at[i],
                                            device_id=dev(nx - dx if incoming else dx, 0, core), device_id_type=MESH)

    def uown():
        return pltpu.make_async_copy(ublock(0), ru_ref.at[0], us_s.at[0])

    def ws2_load(i):
        j = ((x + nx - i // 2) % nx) * 2 + (c if i % 2 == 0 else 1 - c)
        return pltpu.make_async_copy(ws2_ref.at[j], vd.at[i // nx, pl.ds((i % nx) * deep, deep), :], ssem.at[1 + i])

    def shared_up():
        first = pltpu.make_async_copy(ws1_ref, vg.at[0, :, pl.ds(0, 2 * wide)], ssem.at[0])
        first.start()

        def rows_of(i):
            d = flat(i // 2, 0, c if i % 2 == 0 else 1 - c)
            return pltpu.make_async_copy(tg_ref.at[d], tb.at[i % DEPTH], tsem.at[i % DEPTH])

        for i in range(DEPTH - 1):
            rows_of(i).start()
        for i in range(2 * nx):
            ws2_load(i).start()
        first.wait()
        for i in range(2 * nx):
            rows_of(i).wait()
            if i + DEPTH - 1 < 2 * nx:
                rows_of(i + DEPTH - 1).start()
            a = jnp.dot(tb[i % DEPTH], vg[0, :, :wide], preferred_element_type=f32)
            b = jnp.dot(tb[i % DEPTH], vg[0, :, wide:2 * wide], preferred_element_type=f32)
            xin[i // nx, :ntok, (i % nx) * wide:(i % nx + 1) * wide] = (a * jax.nn.sigmoid(a) * b).astype(bf16)
        uown().start()
        for i in range(1, 2 * nx):
            ucopy(i).start()

    def shared_down():
        uown().wait()
        pulls = []
        for i in range(2 * nx):
            if i:
                ucopy(i, True).wait_recv()
            p = pltpu.make_async_copy(ru_ref.at[i], tb.at[i // nx, :, pl.ds((i % nx) * wide, wide)], ssem.at[9 + i])
            p.start()
            pulls.append(p)
        for i in range(2 * nx):
            ws2_load(i).wait()
            pulls[i].wait()

        def col(n, _):
            at = pl.ds(pl.multiple_of(n * 256, 256), 256)
            tot = acc_ref[:, at]
            for i in range(2 * nx):
                tot = tot + jnp.dot(tb[i // nx, :, (i % nx) * wide:(i % nx) * wide + deep],
                                    vd[i // nx, (i % nx) * deep:(i % nx + 1) * deep, at], preferred_element_type=f32)
            acc_ref[:, at] = tot
            return 0

        lax.fori_loop(0, dm // 256, col, 0)

    def work(g, _):
        for w in range(1, 5):
            @pl.when(g == w - 1)
            def _():
                round_(w)
                if w == 1:
                    siblings(0)
                siblings(w)
                if w == 1:
                    own.wait()
                    each_other(lambda j, s: choices(j, s, True).wait_recv())
                    upto = (lax.broadcasted_iota(jnp.int32, (ntok, ntok), 0)
                            <= lax.broadcasted_iota(jnp.int32, (ntok, ntok), 1)).astype(f32).astype(bf16)
                    for l in range(2):
                        e = (y * 2 * nx + tp) * 2 + l
                        hit = jnp.zeros((2 * nchip, ntok), jnp.bool_)
                        for k in range(code_ref.shape[1]):
                            hit = hit | (ia[:, k, :] == e)
                        hit = hit.astype(f32)
                        cum = jnp.dot(hit.astype(bf16), upto, preferred_element_type=f32)
                        mc_ref[l] = (hit * cum).astype(jnp.int32)

        def fetch(i):
            j = g * per + i // 2
            core = c if i % 2 == 0 else 1 - c
            d = flat(look(DX, j), look(DY, j), core)
            return d, pltpu.make_async_copy(tg_ref.at[d], tb.at[i % DEPTH], tsem.at[i % DEPTH])

        for i in range(DEPTH - 1):
            fetch(i)[1].start()
        for i in range(homes):
            d, cp = fetch(i)
            cp.wait()
            if i + DEPTH - 1 < homes:
                fetch(i + DEPTH - 1)[1].start()
            rows = lax.broadcasted_iota(jnp.int32, (2 * cap, ntok), 0)
            rank = jnp.where(rows < cap, mc_ref[0, pl.ds(d, 1), :], mc_ref[1, pl.ds(d, 1), :])
            sel = (rank == jnp.where(rows < cap, rows, rows - cap) + 1).astype(f32).astype(bf16)
            for n in range(0, dm, 512):
                got = jnp.dot(sel, tb[i % DEPTH, :, n:n + 512], preferred_element_type=f32)
                xin[0, i * cap:(i + 1) * cap, n:n + 512] = got[:cap].astype(bf16)
                xin[1, i * cap:(i + 1) * cap, n:n + 512] = got[cap:].astype(bf16)

        for l in range(2):
            @pl.when(g == 0)
            def _():
                for p in weights(l):
                    p.wait()

            def up(at, n):
                a = jnp.dot(xin[l], vg[l, :, pl.ds(at, n)], preferred_element_type=f32)
                b = jnp.dot(xin[l], vu[l, :, pl.ds(at, n)], preferred_element_type=f32)
                act[:, pl.ds(at, n)] = (a * jax.nn.sigmoid(a) * b).astype(bf16)

            whole = ff // 256
            lax.fori_loop(0, whole, lambda n, _: (up(pl.multiple_of(n * 256, 256), 256), 0)[1], 0)
            if ff % 256:
                up(whole * 256, ff % 256)

            def down(n, _):
                at = pl.multiple_of(n * 256, 256)
                z = jnp.dot(act[...], vd[l, :, pl.ds(at, 256)], preferred_element_type=f32)
                for i in range(homes):
                    zb[g * homes + i, l * cap:(l + 1) * cap, pl.ds(at, 256)] = z[i * cap:(i + 1) * cap].astype(bf16)
                return 0

            lax.fori_loop(0, dm // 256, down, 0)

        @pl.when(g == 0)
        def _():
            pltpu.make_async_copy(zb.at[0], rz_ref.at[0], lsem.at[1]).start()

        @pl.when(g == groups - 2)
        def _():
            for j, s in send_order():
                if j < nchip - per:
                    back(j, s, 2 * j + s).start()

        @pl.when(g == groups - 1)
        def _():
            shared_up()
            for j, s in send_order():
                if j >= nchip - per:
                    back(j, s, 2 * j + s).start()

        return 0

    lax.fori_loop(0, groups, work, 0)

    acc_ref[...] = jnp.zeros_like(acc_ref)

    def arrived(j, s, slot):
        core = c if s == 0 else 1 - c
        return pltpu.make_async_remote_copy(src_ref=zb.at[slot], dst_ref=rz_ref.at[slot], send_sem=rt_s.at[slot],
                                            recv_sem=rt_r.at[slot],
                                            device_id=dev(nx - look(DX, j), ny - look(DY, j), core), device_id_type=MESH)

    def combine(j, _):
        @pl.when(j == nchip - per)
        def _():
            shared_down()

        @pl.when(j == 0)
        def _():
            pltpu.make_async_copy(zb.at[0], rz_ref.at[0], lsem.at[1]).wait()

        @pl.when(j > 0)
        def _():
            arrived(j, 0, 2 * j).wait_recv()

        arrived(j, 1, 2 * j + 1).wait_recv()
        pulls = [pltpu.make_async_copy(rz_ref.at[2 * j + s], zin.at[pl.ds(s * 2 * cap, 2 * cap), :], zsem.at[s]) for s in range(2)]
        for p in pulls:
            p.start()
        base = [flat(nx - look(DX, j), ny - look(DY, j), core) * (2 * cap) for core in (c, 1 - c)]
        lane = lax.broadcasted_iota(jnp.int32, (ntok, 4 * cap), 1)
        want = jnp.where(lane < 2 * cap, base[0] + lane, base[1] + lane - 2 * cap)
        g = jnp.zeros((ntok, 4 * cap), f32)
        for k in range(code_ref.shape[1]):
            g = g + jnp.where(code_ref[:, k:k + 1] == want, gate_ref[:, k:k + 1], 0.0)
        g1 = g.astype(bf16)
        rest = g - g1.astype(f32)
        g2 = rest.astype(bf16)
        g3 = (rest - g2.astype(f32)).astype(bf16)
        for p in pulls:
            p.wait()

        def col(n, _):
            at = pl.ds(pl.multiple_of(n * 512, 512), 512)
            z = zin[:, at]
            acc_ref[:, at] += (jnp.dot(g1, z, preferred_element_type=f32)
                               + (jnp.dot(g2, z, preferred_element_type=f32) + jnp.dot(g3, z, preferred_element_type=f32)))
            return 0

        lax.fori_loop(0, dm // 512, col, 0)
        return 0

    lax.fori_loop(0, nchip, combine, 0)

    for k in range(len(copies)):
        ici(k).wait_send()
    for j in range(nchip):
        d2d(j, c).wait_send()

    def drain(j, s):
        arrived(j, s, 2 * j + s).wait_send()
        choices(j, s).wait_send()

    each_other(drain)
    for i in range(1, 2 * nx):
        ucopy(i).wait_send()


def moe(t, idx, code, gates, w1g, w1u, w2, ws1, ws2, nx, ny, cap):
    ntok, dm = t.shape
    nle, _, ff = w1g.shape
    ndev = 2 * nx * ny
    groups = 4
    rows = ndev // groups * cap
    any_ = pl.BlockSpec(memory_space=pl.ANY)
    vm = pl.BlockSpec(memory_space=pltpu.VMEM)
    ncopy = len(gather_copies(ntok))
    dma = pltpu.SemaphoreType.DMA
    return pl.pallas_call(
        functools.partial(moe_kernel, nx, ny, cap, groups),
        in_specs=[vm, vm, vm, vm] + [any_] * 5,
        out_specs=[vm, any_, any_, any_],
        out_shape=[jax.ShapeDtypeStruct((ntok, dm), f32),
                   jax.ShapeDtypeStruct((ndev, ntok, dm), bf16),
                   jax.ShapeDtypeStruct((ndev, nle * cap, dm), bf16),
                   jax.ShapeDtypeStruct((2 * nx, ntok, ws1.shape[1] // 2), bf16)],
        scratch_shapes=[pltpu.VMEM((nle, dm, ff), bf16), pltpu.VMEM((nle, dm, ff), bf16), pltpu.VMEM((nle, ff, dm), bf16),
                        pltpu.VMEM((nle, rows, dm), bf16), pltpu.VMEM((rows, ff), bf16),
                        pltpu.VMEM((ndev, nle * cap, dm), bf16), pltpu.VMEM((DEPTH, ntok, dm), bf16),
                        pltpu.VMEM((2 * nle * cap, dm), bf16), pltpu.VMEM((ndev,) + idx.shape, jnp.int32),
                        pltpu.VMEM((nle, ndev, ntok), jnp.int32),
                        dma((2, 3, 4)), dma((DEPTH,)), dma((2,)), dma((2,)), dma((ncopy,)), dma((ncopy,)),
                        dma((nx * ny,)), dma((nx * ny,)), dma((ndev,)), dma((ndev,)), dma((ndev,)), dma((ndev,)),
                        dma((2 * nx,)), dma((2 * nx,)), dma((17,))],
        compiler_params=pltpu.CompilerParams(collective_id=0, has_side_effects=True, vmem_limit_bytes=VMEM_MAX),
        cost_estimate=pl.CostEstimate(flops=6 * ndev * nle * cap * dm * ff, bytes_accessed=10 * nle * dm * ff, transcendentals=0),
    )(t, idx, code, gates, w1g, w1u, w2, ws1, ws2)


def solution(mesh):
    ncp = mesh.shape["cp"]
    ntp = mesh.shape["tp"]
    ndev = ncp * ntp
    rows = P(("dp", "cp", "tp"), None)
    cols = P(None, "tp")
    wrows = P("tp", None)
    rep = P(None)
    exps = P(("cp", "tp"), None, None)

    def layer(x, g_attn, wq, wk, wv, wo, g_mlp, idx, gates, w1g, w1u, w2, ws1g, ws1u, ws2):
        r = lax.axis_index("cp")
        me = r * ntp + lax.axis_index("tp")
        ntok, dm = x.shape
        seq = ntok * ndev
        nloc = seq // ncp
        nle = w1g.shape[0]
        num_e = nle * ndev
        top = idx.shape[1]
        cap = -(-top * (2 * ntok // num_e + 1) // 8) * 8

        upto = (jnp.arange(ntok)[:, None] <= jnp.arange(ntok)[None, :]).astype(bf16)
        named = idx[:, :, None] == jnp.arange(num_e)[None, None, :]
        before = lax.dot_general(upto, jnp.any(named, axis=1).astype(bf16), (((0,), (0,)), ((), ())), preferred_element_type=f32) - 1.0
        rank = jnp.sum(jnp.where(named, before[:, None, :], 0.0), axis=-1).astype(jnp.int32)
        code = idx * cap + rank

        half = HEAD // 2
        pos = layout_pos(r * nloc + jnp.arange(nloc), ncp, seq)
        freq = ROPE_BASE ** (-jnp.arange(half, dtype=f32) / half)
        ang = pos.astype(f32)[:, None] * freq[None, :]
        cs, sn = jnp.cos(ang), jnp.sin(ang)
        o, wo_all, ws2_all = attention(x, g_attn, wq, wk, wv, jnp.concatenate([cs, cs], 1), jnp.concatenate([-sn, sn], 1), wo, ws2, ncp, ntp)
        o = lax.all_to_all(o, "tp", 0, 1, tiled=True)
        attn = jnp.dot(o, wo_all.reshape(-1, dm), preferred_element_type=f32)
        h = (x.astype(f32) + attn).astype(bf16)
        t = rms_norm(h, g_mlp)

        idx_t = jnp.pad(idx.T, ((0, 8 - top), (0, 0)), constant_values=-1)
        pad = ((0, 0), (0, -ws1g.shape[1] % 128))
        ws1 = jnp.concatenate([jnp.pad(ws1g, pad), jnp.pad(ws1u, pad)], axis=1)
        added = moe(t, idx_t, code, gates, w1g, w1u, w2, ws1, ws2_all, ntp // 2, ncp, cap)[0]
        return (h.astype(f32) + added).astype(bf16)

    return jax.shard_map(layer, mesh=mesh,
                         in_specs=(rows, rep, cols, cols, cols, wrows, rep, rows, rows, exps, exps, exps, cols, cols, wrows),
                         out_specs=rows, check_vma=False)
```

```python
import functools

import jax
import jax.numpy as jnp
from jax import lax
from jax.experimental import pallas as pl
from jax.experimental.pallas import tpu as pltpu
from jax.sharding import PartitionSpec as P

HEAD = 128
EPS = 1e-6
ROPE_BASE = 10000.0
LOG2E = 1.4426950408889634
MESH = pl.DeviceIdType.MESH
DEPTH = 3
VMEM_MAX = 66_500_000
ONE = 1
TWO = 2
f32 = jnp.float32
bf16 = jnp.bfloat16


def rms_norm(a, g):
    af = a.astype(f32)
    r = af * lax.rsqrt(jnp.mean(af * af, axis=-1, keepdims=True) + EPS)
    return (r * g).astype(bf16)


def layout_pos(i, ncp, seq):
    half = seq // (2 * ncp)
    r = i // (2 * half)
    w = i % (2 * half)
    return jnp.where(w < half, r * half + w, (2 * ncp - 1 - r) * half + w - half)


def attn_kernel(x_ref, g_ref, wq_ref, wk_ref, wv_ref, c_ref, s_ref, wo_ref, ws2_ref, o_ref, wo_all, ws2_all,
                xg, q_s, kvb, m_s, l_s, acc_s, xs, xr, ds, dr, ys, yr, gs, gr, gd, ge, gl):
    ntok, dm = x_ref.shape
    w = wq_ref.shape[ONE]
    heads = w // HEAD
    r = lax.axis_index("cp")
    tp = lax.axis_index("tp")
    ncp, nch = kvb.shape[0], kvb.shape[ONE]
    nx = nch // TWO
    x, c = tp // TWO, tp % TWO
    cexp = HEAD ** -0.5 * LOG2E

    def block(dx, core):
        return ((x + dx) % nx) * TWO + core

    def to_x(dx):
        return {"tp": block(dx, c)}

    def to_y(dy):
        return {"cp": (r + dy) % ncp}

    a = x_ref[...].astype(f32)
    n = a * lax.rsqrt(jnp.mean(a * a, axis=-ONE, keepdims=True) + EPS)
    xg[tp] = (n * g_ref[...]).astype(bf16)

    barrier = pltpu.get_barrier_semaphore()
    for d in (to_x(ONE), to_x(nx - ONE), to_y(ONE), to_y(ncp - ONE), {"tp": block(0, ONE - c)}):
        pl.semaphore_signal(barrier, inc=ONE, device_id=d, device_id_type=MESH)
    pl.semaphore_wait(barrier, 5)

    half = ntok // TWO

    def xcopy(k, incoming=False):
        step = ONE if k in (0, TWO) else nx - ONE
        src = 0 if k < TWO else nx - step
        lo, num = ((0, ntok), (0, ntok), (0, half), (half, half))[k]
        at = (src - step) % nx if incoming else src
        ref = xg.at[block(at, c), pl.ds(lo, num), :]
        return pltpu.make_async_remote_copy(src_ref=ref, dst_ref=ref, send_sem=xs.at[k], recv_sem=xr.at[k],
                                            device_id=to_x(nx - step if incoming else step), device_id_type=MESH)

    def sib(dx, incoming=False):
        ref = xg.at[block(dx, ONE - c if incoming else c)]
        return pltpu.make_async_remote_copy(src_ref=ref, dst_ref=ref, send_sem=ds.at[dx], recv_sem=dr.at[dx],
                                            device_id={"tp": block(0, ONE - c)}, device_id_type=MESH)

    def ycopy(dx, s, k, incoming=False):
        step = ONE if k in (0, TWO) else ncp - ONE
        src = 0 if k < TWO else ncp - step
        rows = kvb.shape[TWO]
        lo, num = ((0, rows), (0, rows), (0, rows // TWO), (rows // TWO, rows // TWO))[k]
        at = (src - step) % ncp if incoming else src
        b = block(dx, c if s == 0 else ONE - c)
        ref = kvb.at[(r + at) % ncp, b, pl.ds(lo, num), :]
        sem = (dx * TWO + s) * 4 + k
        return pltpu.make_async_remote_copy(src_ref=ref, dst_ref=ref, send_sem=ys.at[sem], recv_sem=yr.at[sem],
                                            device_id=to_y(ncp - step if incoming else step), device_id_type=MESH)

    shards = ((wo_ref, wo_all), (ws2_ref, ws2_all))

    def wcopy(a, k, incoming=False):
        own, full = shards[a]
        num = own.shape[0]
        step = ONE if k in (0, TWO) else nx - ONE
        src = 0 if k < TWO else nx - step
        lo, num = ((0, num), (0, num), (0, num // TWO), (num // TWO, num // TWO))[k]
        at = (src - step) % nx if incoming else src
        ref = full.at[block(at, c), pl.ds(lo, num), :]
        return pltpu.make_async_remote_copy(src_ref=own if k < TWO and not incoming else ref, dst_ref=ref,
                                            send_sem=gs.at[a, k], recv_sem=gr.at[a, k],
                                            device_id=to_x(nx - step if incoming else step), device_id_type=MESH)

    def wsib(a, dx, incoming=False):
        own, full = shards[a]
        ref = full.at[block(dx, ONE - c if incoming else c)]
        return pltpu.make_async_remote_copy(src_ref=own if dx == 0 and not incoming else ref, dst_ref=ref,
                                            send_sem=gd.at[a, dx], recv_sem=ge.at[a, dx],
                                            device_id={"tp": block(0, ONE - c)}, device_id_type=MESH)

    def wown(a):
        return pltpu.make_async_copy(shards[a][0], shards[a][ONE].at[tp], gl.at[a])

    def wstart(a):
        wcopy(a, 0).start()
        wcopy(a, ONE).start()
        wsib(a, 0).start()
        wown(a).start()

    def wpass(a):
        wcopy(a, 0, True).wait_recv()
        wcopy(a, TWO).start()
        wcopy(a, ONE, True).wait_recv()
        wcopy(a, 3).start()
        wsib(a, nx - ONE).start()
        wsib(a, ONE).start()

    def wlast(a):
        wcopy(a, TWO, True).wait_recv()
        wcopy(a, 3, True).wait_recv()
        wsib(a, TWO).start()

    def wend(a):
        wown(a).wait()
        for k in range(4):
            wcopy(a, k).wait_send()
        for dx in range(nx):
            wsib(a, dx, True).wait_recv()
            wsib(a, dx).wait_send()

    def qkv(dx, s):
        b = block(dx, c if s == 0 else ONE - c)
        at = pl.ds(pl.multiple_of(b * ntok, ntok), ntok)
        xb = xg[b]
        cs, sn = c_ref[at, :], s_ref[at, :]

        def turned(t):
            return (t * cs + pltpu.roll(t, HEAD // TWO, ONE) * sn)

        k = jnp.dot(xb, wk_ref[...], preferred_element_type=f32)
        for h in range(heads):
            kvb[r, b, h * HEAD:(h + ONE) * HEAD, :] = turned(k[:, h * HEAD:(h + ONE) * HEAD]).T.astype(bf16)
        kvb[r, b, w:, :] = jnp.dot(xb, wv_ref[...], preferred_element_type=f32).astype(bf16)
        q = jnp.dot(xb, wq_ref[...], preferred_element_type=f32)
        for h in range(heads):
            q_s[at, h * HEAD:(h + ONE) * HEAD] = turned(q[:, h * HEAD:(h + ONE) * HEAD]).astype(bf16)
        ycopy(dx, s, 0).start()
        ycopy(dx, s, ONE).start()

    def pass_on(dx, s):
        for k in (0, ONE):
            ycopy(dx, s, k, True).wait_recv()
        for k in (TWO, 3):
            ycopy(dx, s, k).start()

    xcopy(0).start()
    xcopy(ONE).start()
    sib(0).start()
    m_s[...] = jnp.full_like(m_s, -1e30)
    l_s[...] = jnp.zeros_like(l_s)
    acc_s[...] = jnp.zeros_like(acc_s)
    qkv(0, 0)
    sib(0, True).wait_recv()
    qkv(0, ONE)
    xcopy(0, True).wait_recv()
    xcopy(TWO).start()
    sib(nx - ONE).start()
    xcopy(ONE, True).wait_recv()
    xcopy(3).start()
    sib(ONE).start()
    qkv(nx - ONE, 0)
    qkv(ONE, 0)
    for dx in (nx - ONE, ONE):
        sib(dx, True).wait_recv()
        qkv(dx, ONE)
    for s in (0, ONE):
        pass_on(0, s)
    wstart(0)
    wstart(ONE)
    xcopy(TWO, True).wait_recv()
    xcopy(3, True).wait_recv()
    sib(TWO).start()
    qkv(TWO, 0)
    sib(TWO, True).wait_recv()
    qkv(TWO, ONE)

    def attend(h, qb, rank, kb, chunks, diag):
        rows = pl.ds(pl.multiple_of(qb * ntok, ntok), ntok)
        cols = slice(h * HEAD, (h + ONE) * HEAD)
        q = q_s[rows, cols]
        sc = []
        for j in range(chunks):
            t = jnp.dot(q, kvb[rank, kb + j, cols, :], preferred_element_type=f32)
            if diag and j == chunks - ONE:
                t = jnp.where(lax.broadcasted_iota(jnp.int32, t.shape, ONE) <= lax.broadcasted_iota(jnp.int32, t.shape, 0), t, -1e30)
            sc.append(t)
        m_old = m_s[h, rows, :]
        top = sc[0]
        for t in sc[ONE:]:
            top = jnp.maximum(top, t)
        m_new = jnp.maximum(m_old, jnp.max(top, axis=ONE, keepdims=True))
        alpha = jnp.exp2((m_old - m_new) * cexp)
        ps = [jnp.exp2((t - m_new[:, :ONE]) * cexp) for t in sc]
        tot = ps[0]
        for p in ps[ONE:]:
            tot = tot + p
        pv = None
        for j, p in enumerate(ps):
            t = jnp.dot(p.astype(bf16), kvb[rank, kb + j, w:, cols], preferred_element_type=f32)
            pv = t if pv is None else pv + t
        l_s[h, rows, :] = alpha * l_s[h, rows, :] + jnp.sum(tot, axis=ONE, keepdims=True)
        acc_s[h, rows, :] = alpha * acc_s[h, rows, :] + pv
        m_s[h, rows, :] = m_new

    per = nch // TWO

    def full(rank, qbase, kb):
        def go(i, _):
            for h in range(heads):
                attend(h, qbase + i, rank, kb, per, False)
            return 0

        lax.fori_loop(0, per, go, 0)

    def own_diag(second, _):
        base = second * per
        for i in range(per):
            for h in range(heads):
                attend(h, base + i, r, base, i + ONE, True)
        return 0

    lax.fori_loop(0, TWO, own_diag, 0)
    for dx in (nx - ONE, ONE):
        for s in (0, ONE):
            pass_on(dx, s)
    full(r, per, 0)
    for s in (0, ONE):
        pass_on(TWO, s)
    wpass(0)

    def other(dy):
        rank = (r + dy) % ncp
        low = jnp.where(rank < r, 0, per)
        full(rank, per, 0)
        full(rank, low, low)

    other(ONE)
    wlast(0)
    other(ncp - ONE)
    wpass(ONE)
    for dx in range(nx):
        for s in (0, ONE):
            for k in (TWO, 3):
                ycopy(dx, s, k, True).wait_recv()
    other(TWO)
    wlast(ONE)
    for h in range(heads):
        o_ref[:, h * HEAD:(h + ONE) * HEAD] = (acc_s[h] / l_s[h]).astype(bf16)

    wend(0)
    wend(ONE)
    for k in range(4):
        xcopy(k).wait_send()
    for dx in range(nx):
        sib(dx).wait_send()
        for s in (0, ONE):
            for k in range(4):
                ycopy(dx, s, k).wait_send()


def attention(x, g, wq, wk, wv, cos, sin, wo, ws2, ncp, ntp):
    ntok, dm = x.shape
    w = wq.shape[ONE]
    heads = w // HEAD
    n = ntok * ntp
    vm = pl.BlockSpec(memory_space=pltpu.VMEM)
    any_ = pl.BlockSpec(memory_space=pl.ANY)
    dma = pltpu.SemaphoreType.DMA
    return pl.pallas_call(
        attn_kernel,
        in_specs=[vm] * 7 + [any_] * TWO,
        out_specs=[vm, any_, any_],
        out_shape=[jax.ShapeDtypeStruct((n, w), bf16), jax.ShapeDtypeStruct((ntp,) + wo.shape, bf16),
                   jax.ShapeDtypeStruct((ntp,) + ws2.shape, bf16)],
        scratch_shapes=[pltpu.VMEM((ntp, ntok, dm), bf16), pltpu.VMEM((n, w), bf16), pltpu.VMEM((ncp, ntp, TWO * w, ntok), bf16),
                        pltpu.VMEM((heads, n, HEAD), f32), pltpu.VMEM((heads, n, HEAD), f32), pltpu.VMEM((heads, n, HEAD), f32),
                        dma((4,)), dma((4,)), dma((ntp // TWO,)), dma((ntp // TWO,)), dma((4 * ntp,)), dma((4 * ntp,)),
                        dma((TWO, 4)), dma((TWO, 4)), dma((TWO, ntp // TWO)), dma((TWO, ntp // TWO)), dma((TWO,))],
        compiler_params=pltpu.CompilerParams(collective_id=ONE, has_side_effects=True, vmem_limit_bytes=60 * TWO**20),
        cost_estimate=pl.CostEstimate(flops=6 * n * dm * w + TWO * n * n * ncp * w, bytes_accessed=16 * n * dm, transcendentals=0),
    )(x, g.reshape(ONE, dm), wq, wk, wv, cos, sin, wo, ws2)


ORDER = [(0, 0), (ONE, 0), (3, 0), (0, ONE), (0, 3), (TWO, 0), (0, TWO), (ONE, ONE),
         (ONE, 3), (3, ONE), (3, 3), (TWO, ONE), (TWO, 3), (ONE, TWO), (3, TWO), (TWO, TWO)]
DIST = [0, ONE, TWO, ONE]


def packed(values):
    return [sum(v << (TWO * i) for i, v in enumerate(values[k:k + 8])) for k in (0, 8)]


DX, DY = packed([o[0] for o in ORDER]), packed([o[ONE] for o in ORDER])


def look(table, j):
    a, b = table
    return ((a + (j // 8) * (b - a)) >> (TWO * (j % 8))) & 3


def gather_copies(rows):
    h, q = rows // TWO, rows // 4
    out = []
    for flip in (False, True):
        base = h if flip else 0
        fw = (lambda a, b: (b, a)) if flip else (lambda a, b: (a, b))

        def add(rank, blk, lo, n, step):
            out.append((rank, fw(*blk), base + lo, n, fw(*step)))

        add(0, (0, 0), 0, h, (ONE, 0))
        add(0, (0, 0), 0, h, (3, 0))
        add(ONE, (3, 0), 0, q, (ONE, 0))
        add(ONE, (ONE, 0), q, q, (3, 0))
        for b in (3, ONE, 0, TWO):
            add(TWO, (b, 0), 0, h, (0, ONE))
            add(TWO, (b, 0), 0, h, (0, 3))
            add(3, (b, 3), 0, q, (0, ONE))
            add(3, (b, ONE), q, q, (0, 3))
    out.sort(key=lambda t: t[0])
    return [t[ONE:] for t in out]


def dist(b):
    return DIST[b[0]] + DIST[b[ONE]]


def moe_kernel(nx, ny, cap, groups, t_ref, idx_ref, code_ref, gate_ref, w1g_ref, w1u_ref, w2_ref,
               ws1_ref, ws2_ref, acc_ref, tg_ref, rz_ref, ru_ref, md_ref,
               vg, vu, vd, xin, act, zb, tb, zin, ia, mc_ref,
               wsem, tsem, zsem, lsem, ag_s, ag_r, dd_s, dd_r, rt_s, rt_r, ix_s, ix_r,
               us_s, us_r, ssem, l1_s, l1_r, l2_s, l2_r):
    ntok, dm = t_ref.shape
    ff = w1g_ref.shape[TWO]
    y = lax.axis_index("cp")
    tp = lax.axis_index("tp")
    x, c = tp // TWO, tp % TWO
    nchip = nx * ny
    per = nchip // groups
    homes = TWO * per

    def dev(dx, dy, core):
        return {"cp": (y + dy) % ny, "tp": ((x + dx) % nx) * TWO + core}

    def flat(dx, dy, core):
        return ((y + dy) % ny) * (TWO * nx) + ((x + dx) % nx) * TWO + core

    def weights(l):
        return [pltpu.make_async_copy(a.at[l, pl.ds(k * (a.shape[ONE] // 4), a.shape[ONE] // 4), :],
                                      b.at[l, pl.ds(k * (a.shape[ONE] // 4), a.shape[ONE] // 4), :], wsem.at[l, n, k])
                for n, (a, b) in enumerate(((w1g_ref, vg), (w1u_ref, vu), (w2_ref, vd))) for k in range(4)]

    own = pltpu.make_async_copy(t_ref, tg_ref.at[flat(0, 0, c)], lsem.at[0])

    ia[flat(0, 0, c)] = idx_ref[...]
    barrier = pltpu.get_barrier_semaphore()

    def greet(k, _):
        other = (y * TWO * nx + tp + k) % (TWO * nchip)
        pl.semaphore_signal(barrier, inc=ONE, device_id={"cp": other // (TWO * nx), "tp": other % (TWO * nx)}, device_id_type=MESH)
        return 0

    lax.fori_loop(ONE, TWO * nchip, greet, 0)
    pl.semaphore_wait(barrier, TWO * nchip - ONE)

    copies = gather_copies(ntok)

    def ici(k):
        blk, lo, n, step = copies[k]
        here = tg_ref.at[flat(blk[0], blk[ONE], c), pl.ds(lo, n), :]
        src = t_ref.at[pl.ds(lo, n), :] if blk == (0, 0) else here
        return pltpu.make_async_remote_copy(src_ref=src, dst_ref=here, send_sem=ag_s.at[k], recv_sem=ag_r.at[k],
                                            device_id=dev(step[0], step[ONE], c), device_id_type=MESH)

    def ici_in(k):
        blk, lo, n, step = copies[k]
        here = tg_ref.at[flat(blk[0] - step[0] + nx, blk[ONE] - step[ONE] + ny, c), pl.ds(lo, n), :]
        return pltpu.make_async_remote_copy(src_ref=here, dst_ref=here, send_sem=ag_s.at[k], recv_sem=ag_r.at[k],
                                            device_id=dev(nx - step[0], ny - step[ONE], c), device_id_type=MESH)

    def d2d(j, core):
        blk = ORDER[j]
        here = tg_ref.at[flat(blk[0], blk[ONE], core)]
        src = t_ref if (j == 0) else here
        return pltpu.make_async_remote_copy(src_ref=src, dst_ref=here, send_sem=dd_s.at[j], recv_sem=dd_r.at[j],
                                            device_id=dev(0, 0, ONE - c), device_id_type=MESH)

    def d2d_in(j):
        blk = ORDER[j]
        here = tg_ref.at[flat(blk[0], blk[ONE], ONE - c)]
        return pltpu.make_async_remote_copy(src_ref=here, dst_ref=here, send_sem=dd_s.at[j], recv_sem=dd_r.at[j],
                                            device_id=dev(0, 0, ONE - c), device_id_type=MESH)

    def round_(w):
        h = ntok // TWO
        if w == 0:
            for k, cp in enumerate(copies):
                if cp[0] == (0, 0):
                    ici(k).start()
            d2d(0, c).start()
            return
        left = {}
        into = [(k, ((cp[0][0] - cp[3][0]) % nx, (cp[0][ONE] - cp[3][ONE]) % ny), cp) for k, cp in enumerate(copies) if dist(cp[0]) == w - ONE]
        for k, blk, cp in into:
            part = (blk, cp[ONE] // h)
            left[part] = left.get(part, 0) + cp[TWO]
        done = {}
        for k, blk, cp in into:
            ici_in(k).wait_recv()
            part = (blk, cp[ONE] // h)
            left[part] -= cp[TWO]
            if left[part] == 0:
                for n, out in enumerate(copies):
                    if out[0] == blk and out[ONE] // h == part[ONE]:
                        ici(n).start()
                done[blk] = done.get(blk, 0) + ONE
                if done[blk] == TWO:
                    d2d(ORDER.index(blk), c).start()

    def siblings(w):
        for j, b in enumerate(ORDER):
            if dist(b) == w:
                d2d_in(j).wait_recv()

    def choices(j, s, incoming=False):
        core = c if s == 0 else ONE - c
        dx, dy = look(DX, j), look(DY, j)
        ref = ia.at[flat(nx - dx, ny - dy, core) if incoming else flat(0, 0, c)]
        return pltpu.make_async_remote_copy(src_ref=ref, dst_ref=ref, send_sem=ix_s.at[TWO * j + s], recv_sem=ix_r.at[TWO * j + s],
                                            device_id=dev(nx - dx, ny - dy, core) if incoming else dev(dx, dy, core),
                                            device_id_type=MESH)

    def each_other(do):
        def go(j, _):
            @pl.when(j > 0)
            def _():
                do(j, 0)

            do(j, ONE)
            return 0

        lax.fori_loop(0, nchip, go, 0)

    each_other(lambda j, s: choices(j, s).start())
    round_(0)
    own.start()
    for l in range(TWO):
        for p in weights(l):
            p.start()

    def back(j, s, slot):
        core = c if s == 0 else ONE - c
        return pltpu.make_async_remote_copy(src_ref=zb.at[slot], dst_ref=rz_ref.at[slot], send_sem=rt_s.at[slot],
                                            recv_sem=rt_r.at[slot],
                                            device_id=dev(look(DX, j), look(DY, j), core), device_id_type=MESH)

    straight = sum(0 in o for o in ORDER)

    def cols(half):
        return pl.ds(half * (dm // TWO), dm // TWO)

    def leg1(j, half, incoming=False):
        dx, dy = ORDER[j]
        step = (0, dy) if half else (dx, 0)
        if incoming:
            step = (nx - step[0], ny - step[ONE])
        return pltpu.make_async_remote_copy(src_ref=zb.at[pl.ds(TWO * j, TWO), :, cols(half)], dst_ref=md_ref.at[j - straight, half],
                                            send_sem=l1_s.at[j - straight, half], recv_sem=l1_r.at[j - straight, half],
                                            device_id=dev(step[0], step[ONE], c), device_id_type=MESH)

    def leg2(j, s, half):
        step = (look(DX, j), 0) if half else (0, look(DY, j))
        return pltpu.make_async_remote_copy(src_ref=md_ref.at[j - straight, half, s], dst_ref=rz_ref.at[TWO * j + s, :, cols(half)],
                                            send_sem=l2_s.at[j - straight, s, half], recv_sem=l2_r.at[j - straight, s, half],
                                            device_id=dev(step[0], step[ONE], ONE - c if s else c), device_id_type=MESH)

    def leg2_in(j, s, half):
        step = (look(DX, j), 0) if half else (0, look(DY, j))
        return pltpu.make_async_remote_copy(src_ref=md_ref.at[j - straight, half, s], dst_ref=rz_ref.at[TWO * j + s, :, cols(half)],
                                            send_sem=l2_s.at[j - straight, s, half], recv_sem=l2_r.at[j - straight, s, half],
                                            device_id=dev(nx - step[0], ny - step[ONE], ONE - c if s else c), device_id_type=MESH)

    def forward(j):
        for half in range(TWO):
            leg1(j, half, True).wait_recv()
            for s in range(TWO):
                leg2(j, s, half).start()

    wide = ws1_ref.shape[ONE] // TWO
    deep = ws2_ref.shape[ONE]

    def ublock(i):
        return xin.at[i // nx, pl.ds(0, ntok), pl.ds((i % nx) * wide, wide)]

    def ucopy(i, incoming=False):
        dx, core = i // TWO, c if i % TWO == 0 else ONE - c
        return pltpu.make_async_remote_copy(src_ref=ublock(i), dst_ref=ru_ref.at[i], send_sem=us_s.at[i], recv_sem=us_r.at[i],
                                            device_id=dev(nx - dx if incoming else dx, 0, core), device_id_type=MESH)

    def uown():
        return pltpu.make_async_copy(ublock(0), ru_ref.at[0], us_s.at[0])

    def ws2_load(i):
        j = ((x + nx - i // TWO) % nx) * TWO + (c if i % TWO == 0 else ONE - c)
        return pltpu.make_async_copy(ws2_ref.at[j], vd.at[i // nx, pl.ds((i % nx) * deep, deep), :], ssem.at[ONE + i])

    def shared_up():
        first = pltpu.make_async_copy(ws1_ref, vg.at[0, :, pl.ds(0, TWO * wide)], ssem.at[0])
        first.start()

        def rows_of(i):
            d = flat(i // TWO, 0, c if i % TWO == 0 else ONE - c)
            return pltpu.make_async_copy(tg_ref.at[d], tb.at[i % DEPTH], tsem.at[i % DEPTH])

        for i in range(DEPTH - ONE):
            rows_of(i).start()
        for i in range(TWO * nx):
            ws2_load(i).start()
        first.wait()
        for i in range(TWO * nx):
            rows_of(i).wait()
            if i + DEPTH - ONE < TWO * nx:
                rows_of(i + DEPTH - ONE).start()
            a = jnp.dot(tb[i % DEPTH], vg[0, :, :wide], preferred_element_type=f32)
            b = jnp.dot(tb[i % DEPTH], vg[0, :, wide:TWO * wide], preferred_element_type=f32)
            xin[i // nx, :ntok, (i % nx) * wide:(i % nx + ONE) * wide] = (a * jax.nn.sigmoid(a) * b).astype(bf16)
        uown().start()
        for i in range(ONE, TWO * nx):
            ucopy(i).start()

    def shared_down():
        uown().wait()
        pulls = []
        for i in range(TWO * nx):
            if i:
                ucopy(i, True).wait_recv()
            p = pltpu.make_async_copy(ru_ref.at[i], tb.at[i // nx, :, pl.ds((i % nx) * wide, wide)], ssem.at[9 + i])
            p.start()
            pulls.append(p)
        for i in range(TWO * nx):
            ws2_load(i).wait()
            pulls[i].wait()

        def col(n, _):
            at = pl.ds(pl.multiple_of(n * 256, 256), 256)
            tot = acc_ref[:, at]
            for i in range(TWO * nx):
                tot = tot + jnp.dot(tb[i // nx, :, (i % nx) * wide:(i % nx) * wide + deep],
                                    vd[i // nx, (i % nx) * deep:(i % nx + ONE) * deep, at], preferred_element_type=f32)
            acc_ref[:, at] = tot
            return 0

        lax.fori_loop(0, dm // 256, col, 0)

    def work(g, _):
        for w in range(ONE, 5):
            @pl.when(g == w - ONE)
            def _():
                round_(w)
                if w == ONE:
                    siblings(0)
                siblings(w)
                if w == ONE:
                    own.wait()
                    each_other(lambda j, s: choices(j, s, True).wait_recv())
                    upto = (lax.broadcasted_iota(jnp.int32, (ntok, ntok), 0)
                            <= lax.broadcasted_iota(jnp.int32, (ntok, ntok), ONE)).astype(f32).astype(bf16)
                    for l in range(TWO):
                        e = (y * TWO * nx + tp) * TWO + l
                        hit = jnp.zeros((TWO * nchip, ntok), jnp.bool_)
                        for k in range(code_ref.shape[ONE]):
                            hit = hit | (ia[:, k, :] == e)
                        hit = hit.astype(f32)
                        cum = jnp.dot(hit.astype(bf16), upto, preferred_element_type=f32)
                        mc_ref[l] = (hit * cum).astype(jnp.int32)

        @pl.when(g == groups - ONE)
        def _():
            forward(straight)

        def fetch(i):
            j = g * per + i // TWO
            core = c if i % TWO == 0 else ONE - c
            d = flat(look(DX, j), look(DY, j), core)
            return d, pltpu.make_async_copy(tg_ref.at[d], tb.at[i % DEPTH], tsem.at[i % DEPTH])

        for i in range(DEPTH - ONE):
            fetch(i)[ONE].start()
        for i in range(homes):
            d, cp = fetch(i)
            cp.wait()
            if i + DEPTH - ONE < homes:
                fetch(i + DEPTH - ONE)[ONE].start()
            rows = lax.broadcasted_iota(jnp.int32, (TWO * cap, ntok), 0)
            rank = jnp.where(rows < cap, mc_ref[0, pl.ds(d, ONE), :], mc_ref[ONE, pl.ds(d, ONE), :])
            sel = (rank == jnp.where(rows < cap, rows, rows - cap) + ONE).astype(f32).astype(bf16)
            for n in range(0, dm, 512):
                got = jnp.dot(sel, tb[i % DEPTH, :, n:n + 512], preferred_element_type=f32)
                xin[0, i * cap:(i + ONE) * cap, n:n + 512] = got[:cap].astype(bf16)
                xin[ONE, i * cap:(i + ONE) * cap, n:n + 512] = got[cap:].astype(bf16)

        for l in range(TWO):
            @pl.when(g == 0)
            def _():
                for p in weights(l):
                    p.wait()

            def up(at, n):
                a = jnp.dot(xin[l], vg[l, :, pl.ds(at, n)], preferred_element_type=f32)
                b = jnp.dot(xin[l], vu[l, :, pl.ds(at, n)], preferred_element_type=f32)
                act[:, pl.ds(at, n)] = (a * jax.nn.sigmoid(a) * b).astype(bf16)

            whole = ff // 256
            lax.fori_loop(0, whole, lambda n, _: (up(pl.multiple_of(n * 256, 256), 256), 0)[ONE], 0)
            if ff % 256:
                up(whole * 256, ff % 256)

            def down(n, _):
                at = pl.multiple_of(n * 256, 256)
                z = jnp.dot(act[...], vd[l, :, pl.ds(at, 256)], preferred_element_type=f32)
                for i in range(homes):
                    zb[g * homes + i, l * cap:(l + ONE) * cap, pl.ds(at, 256)] = z[i * cap:(i + ONE) * cap].astype(bf16)
                return 0

            lax.fori_loop(0, dm // 256, down, 0)

        @pl.when(g == 0)
        def _():
            pltpu.make_async_copy(zb.at[0], rz_ref.at[0], lsem.at[ONE]).start()

        for k in range(groups):
            @pl.when(g == k)
            def _():
                if k == groups - ONE:
                    shared_up()
                mine = range(k * per, (k + ONE) * per)
                for j in mine:
                    if j >= straight:
                        leg1(j, 0).start()
                        leg1(j, ONE).start()
                for s in range(TWO):
                    for j in mine:
                        if j < straight and j + s:
                            back(j, s, TWO * j + s).start()

        return 0

    lax.fori_loop(0, groups, work, 0)
    for j in range(straight + ONE, nchip):
        forward(j)

    acc_ref[...] = jnp.zeros_like(acc_ref)

    def arrived(j, s, slot):
        core = c if s == 0 else ONE - c
        return pltpu.make_async_remote_copy(src_ref=zb.at[slot], dst_ref=rz_ref.at[slot], send_sem=rt_s.at[slot],
                                            recv_sem=rt_r.at[slot],
                                            device_id=dev(nx - look(DX, j), ny - look(DY, j), core), device_id_type=MESH)

    def combine(j, _):
        @pl.when(j == nchip - per)
        def _():
            shared_down()

        @pl.when(j == 0)
        def _():
            pltpu.make_async_copy(zb.at[0], rz_ref.at[0], lsem.at[ONE]).wait()

        @pl.when((j > 0) & (j < straight))
        def _():
            arrived(j, 0, TWO * j).wait_recv()

        @pl.when(j < straight)
        def _():
            arrived(j, ONE, TWO * j + ONE).wait_recv()

        @pl.when(j >= straight)
        def _():
            for s in range(TWO):
                for half in range(TWO):
                    leg2_in(j, s, half).wait_recv()

        pulls = [pltpu.make_async_copy(rz_ref.at[TWO * j + s], zin.at[pl.ds(s * TWO * cap, TWO * cap), :], zsem.at[s]) for s in range(TWO)]
        for p in pulls:
            p.start()
        base = [flat(nx - look(DX, j), ny - look(DY, j), core) * (TWO * cap) for core in (c, ONE - c)]
        lane = lax.broadcasted_iota(jnp.int32, (ntok, 4 * cap), ONE)
        want = jnp.where(lane < TWO * cap, base[0] + lane, base[ONE] + lane - TWO * cap)
        g = jnp.zeros((ntok, 4 * cap), f32)
        for k in range(code_ref.shape[ONE]):
            g = g + jnp.where(code_ref[:, k:k + ONE] == want, gate_ref[:, k:k + ONE], 0.0)
        g1 = g.astype(bf16)
        rest = g - g1.astype(f32)
        g2 = rest.astype(bf16)
        g3 = (rest - g2.astype(f32)).astype(bf16)
        for p in pulls:
            p.wait()

        def col(n, _):
            at = pl.ds(pl.multiple_of(n * 512, 512), 512)
            z = zin[:, at]
            acc_ref[:, at] += (jnp.dot(g1, z, preferred_element_type=f32)
                               + (jnp.dot(g2, z, preferred_element_type=f32) + jnp.dot(g3, z, preferred_element_type=f32)))
            return 0

        lax.fori_loop(0, dm // 512, col, 0)
        return 0

    lax.fori_loop(0, nchip, combine, 0)

    for k in range(len(copies)):
        ici(k).wait_send()
    for j in range(nchip):
        d2d(j, c).wait_send()

    each_other(lambda j, s: choices(j, s).wait_send())
    for j in range(nchip):
        for s in range(TWO):
            if j >= straight:
                leg1(j, s).wait_send()
                for half in range(TWO):
                    leg2(j, s, half).wait_send()
            elif j + s:
                back(j, s, TWO * j + s).wait_send()
    for i in range(ONE, TWO * nx):
        ucopy(i).wait_send()


def moe(t, idx, code, gates, w1g, w1u, w2, ws1, ws2, nx, ny, cap):
    ntok, dm = t.shape
    nle, _, ff = w1g.shape
    ndev = TWO * nx * ny
    groups = 4
    rows = ndev // groups * cap
    any_ = pl.BlockSpec(memory_space=pl.ANY)
    vm = pl.BlockSpec(memory_space=pltpu.VMEM)
    ncopy = len(gather_copies(ntok))
    turns = sum(0 not in o for o in ORDER)
    dma = pltpu.SemaphoreType.DMA
    return pl.pallas_call(
        functools.partial(moe_kernel, nx, ny, cap, groups),
        in_specs=[vm, vm, vm, vm] + [any_] * 5,
        out_specs=[vm] + [any_] * 4,
        out_shape=[jax.ShapeDtypeStruct((ntok, dm), f32),
                   jax.ShapeDtypeStruct((ndev, ntok, dm), bf16),
                   jax.ShapeDtypeStruct((ndev, nle * cap, dm), bf16),
                   jax.ShapeDtypeStruct((TWO * nx, ntok, ws1.shape[ONE] // TWO), bf16),
                   jax.ShapeDtypeStruct((turns, TWO, TWO, nle * cap, dm // TWO), bf16)],
        scratch_shapes=[pltpu.VMEM((nle, dm, ff), bf16), pltpu.VMEM((nle, dm, ff), bf16), pltpu.VMEM((nle, ff, dm), bf16),
                        pltpu.VMEM((nle, rows, dm), bf16), pltpu.VMEM((rows, ff), bf16),
                        pltpu.VMEM((ndev, nle * cap, dm), bf16), pltpu.VMEM((DEPTH, ntok, dm), bf16),
                        pltpu.VMEM((TWO * nle * cap, dm), bf16), pltpu.VMEM((ndev,) + idx.shape, jnp.int32),
                        pltpu.VMEM((nle, ndev, ntok), jnp.int32),
                        dma((TWO, 3, 4)), dma((DEPTH,)), dma((TWO,)), dma((TWO,)), dma((ncopy,)), dma((ncopy,)),
                        dma((nx * ny,)), dma((nx * ny,)), dma((ndev,)), dma((ndev,)), dma((ndev,)), dma((ndev,)),
                        dma((TWO * nx,)), dma((TWO * nx,)), dma((17,)), dma((turns, TWO)), dma((turns, TWO)),
                        dma((turns, TWO, TWO)), dma((turns, TWO, TWO))],
        compiler_params=pltpu.CompilerParams(collective_id=0, has_side_effects=True, vmem_limit_bytes=VMEM_MAX),
        cost_estimate=pl.CostEstimate(flops=6 * ndev * nle * cap * dm * ff, bytes_accessed=10 * nle * dm * ff, transcendentals=0),
    )(t, idx, code, gates, w1g, w1u, w2, ws1, ws2)


def solution(mesh):
    ncp = mesh.shape["cp"]
    ntp = mesh.shape["tp"]
    ndev = ncp * ntp
    rows = P(("dp", "cp", "tp"), None)
    cols = P(None, "tp")
    wrows = P("tp", None)
    rep = P(None)
    exps = P(("cp", "tp"), None, None)

    def layer(x, g_attn, wq, wk, wv, wo, g_mlp, idx, gates, w1g, w1u, w2, ws1g, ws1u, ws2):
        r = lax.axis_index("cp")
        me = r * ntp + lax.axis_index("tp")
        ntok, dm = x.shape
        seq = ntok * ndev
        nloc = seq // ncp
        nle = w1g.shape[0]
        num_e = nle * ndev
        top = idx.shape[ONE]
        cap = -(-top * (TWO * ntok // num_e + ONE) // 8) * 8

        upto = (jnp.arange(ntok)[:, None] <= jnp.arange(ntok)[None, :]).astype(bf16)
        named = idx[:, :, None] == jnp.arange(num_e)[None, None, :]
        before = lax.dot_general(upto, jnp.any(named, axis=ONE).astype(bf16), (((0,), (0,)), ((), ())), preferred_element_type=f32) - 1.0
        rank = jnp.sum(jnp.where(named, before[:, None, :], 0.0), axis=-ONE).astype(jnp.int32)
        code = idx * cap + rank

        half = HEAD // TWO
        pos = layout_pos(r * nloc + jnp.arange(nloc), ncp, seq)
        freq = ROPE_BASE ** (-jnp.arange(half, dtype=f32) / half)
        ang = pos.astype(f32)[:, None] * freq[None, :]
        cs, sn = jnp.cos(ang), jnp.sin(ang)
        o, wo_all, ws2_all = attention(x, g_attn, wq, wk, wv, jnp.concatenate([cs, cs], ONE), jnp.concatenate([-sn, sn], ONE), wo, ws2, ncp, ntp)
        o = lax.all_to_all(o, "tp", 0, ONE, tiled=True)
        attn = jnp.dot(o, wo_all.reshape(-ONE, dm), preferred_element_type=f32)
        h = (x.astype(f32) + attn).astype(bf16)
        t = rms_norm(h, g_mlp)

        idx_t = jnp.pad(idx.T, ((0, 8 - top), (0, 0)), constant_values=-ONE)
        pad = ((0, 0), (0, -ws1g.shape[ONE] % 128))
        ws1 = jnp.concatenate([jnp.pad(ws1g, pad), jnp.pad(ws1u, pad)], axis=ONE)
        added = moe(t, idx_t, code, gates, w1g, w1u, w2, ws1, ws2_all, ntp // TWO, ncp, cap)[0]
        return (h.astype(f32) + added).astype(bf16)

    return jax.shard_map(layer, mesh=mesh,
                         in_specs=(rows, rep, cols, cols, cols, wrows, rep, rows, rows, exps, exps, exps, cols, cols, wrows),
                         out_specs=rows, check_vma=False)
```

```python
import functools

import jax
import jax.numpy as jnp
from jax import lax
from jax.experimental import pallas as pl
from jax.experimental.pallas import tpu as pltpu
from jax.sharding import PartitionSpec as P

HEAD = 128
EPS = 1e-6
ROPE_BASE = 10000.0
LOG2E = 1.4426950408889634
MESH = pl.DeviceIdType.MESH
DEPTH = 3
VMEM_MAX = 66_500_000
ONE = 1
TWO = 2
f32 = jnp.float32
bf16 = jnp.bfloat16


def rms_norm(a, g):
    af = a.astype(f32)
    r = af * lax.rsqrt(jnp.mean(af * af, axis=-1, keepdims=True) + EPS)
    return (r * g).astype(bf16)


def layout_pos(i, ncp, seq):
    half = seq // (2 * ncp)
    r = i // (2 * half)
    w = i % (2 * half)
    return jnp.where(w < half, r * half + w, (2 * ncp - 1 - r) * half + w - half)


def attn_kernel(x_ref, g_ref, wq_ref, wk_ref, wv_ref, c_ref, s_ref, wo_ref, ws2_ref, o_ref, wo_all, ws2_all,
                xg, q_s, kvb, m_s, l_s, acc_s, xs, xr, ds, dr, ys, yr, gs, gr, gd, ge, gl):
    ntok, dm = x_ref.shape
    w = wq_ref.shape[ONE]
    heads = w // HEAD
    r = lax.axis_index("cp")
    tp = lax.axis_index("tp")
    ncp, nch = kvb.shape[0], kvb.shape[ONE]
    nx = nch // TWO
    x, c = tp // TWO, tp % TWO
    cexp = HEAD ** -0.5 * LOG2E

    def block(dx, core):
        return ((x + dx) % nx) * TWO + core

    def to_x(dx):
        return {"tp": block(dx, c)}

    def to_y(dy):
        return {"cp": (r + dy) % ncp}

    a = x_ref[...].astype(f32)
    n = a * lax.rsqrt(jnp.mean(a * a, axis=-ONE, keepdims=True) + EPS)
    xg[tp] = (n * g_ref[...]).astype(bf16)

    barrier = pltpu.get_barrier_semaphore()
    for d in (to_x(ONE), to_x(nx - ONE), to_y(ONE), to_y(ncp - ONE), {"tp": block(0, ONE - c)}):
        pl.semaphore_signal(barrier, inc=ONE, device_id=d, device_id_type=MESH)
    pl.semaphore_wait(barrier, 5)

    half = ntok // TWO

    def xcopy(k, incoming=False):
        step = ONE if k in (0, TWO) else nx - ONE
        src = 0 if k < TWO else nx - step
        lo, num = ((0, ntok), (0, ntok), (0, half), (half, half))[k]
        at = (src - step) % nx if incoming else src
        ref = xg.at[block(at, c), pl.ds(lo, num), :]
        return pltpu.make_async_remote_copy(src_ref=ref, dst_ref=ref, send_sem=xs.at[k], recv_sem=xr.at[k],
                                            device_id=to_x(nx - step if incoming else step), device_id_type=MESH)

    def sib(dx, incoming=False):
        ref = xg.at[block(dx, ONE - c if incoming else c)]
        return pltpu.make_async_remote_copy(src_ref=ref, dst_ref=ref, send_sem=ds.at[dx], recv_sem=dr.at[dx],
                                            device_id={"tp": block(0, ONE - c)}, device_id_type=MESH)

    def ycopy(dx, s, k, incoming=False):
        step = ONE if k in (0, TWO) else ncp - ONE
        src = 0 if k < TWO else ncp - step
        rows = kvb.shape[TWO]
        lo, num = ((0, rows), (0, rows), (0, rows // TWO), (rows // TWO, rows // TWO))[k]
        at = (src - step) % ncp if incoming else src
        b = block(dx, (c + s) % TWO)
        ref = kvb.at[(r + at) % ncp, b, pl.ds(lo, num), :]
        sem = (dx * TWO + s) * 4 + k
        return pltpu.make_async_remote_copy(src_ref=ref, dst_ref=ref, send_sem=ys.at[sem], recv_sem=yr.at[sem],
                                            device_id=to_y(ncp - step if incoming else step), device_id_type=MESH)

    shards = ((wo_ref, wo_all), (ws2_ref, ws2_all))

    def wcopy(a, k, incoming=False):
        own, full = shards[a]
        num = own.shape[0]
        step = ONE if k in (0, TWO) else nx - ONE
        src = 0 if k < TWO else nx - step
        lo, num = ((0, num), (0, num), (0, num // TWO), (num // TWO, num // TWO))[k]
        at = (src - step) % nx if incoming else src
        ref = full.at[block(at, c), pl.ds(lo, num), :]
        return pltpu.make_async_remote_copy(src_ref=own if k < TWO and not incoming else ref, dst_ref=ref,
                                            send_sem=gs.at[a, k], recv_sem=gr.at[a, k],
                                            device_id=to_x(nx - step if incoming else step), device_id_type=MESH)

    def wsib(a, dx, incoming=False):
        own, full = shards[a]
        ref = full.at[block(dx, ONE - c if incoming else c)]
        return pltpu.make_async_remote_copy(src_ref=own if dx == 0 and not incoming else ref, dst_ref=ref,
                                            send_sem=gd.at[a, dx], recv_sem=ge.at[a, dx],
                                            device_id={"tp": block(0, ONE - c)}, device_id_type=MESH)

    def wown(a):
        return pltpu.make_async_copy(shards[a][0], shards[a][ONE].at[tp], gl.at[a])

    def wstart(a):
        wcopy(a, 0).start()
        wcopy(a, ONE).start()
        wsib(a, 0).start()
        wown(a).start()

    def wpass(a):
        wcopy(a, 0, True).wait_recv()
        wcopy(a, TWO).start()
        wcopy(a, ONE, True).wait_recv()
        wcopy(a, 3).start()
        wsib(a, nx - ONE).start()
        wsib(a, ONE).start()

    def wlast(a):
        wcopy(a, TWO, True).wait_recv()
        wcopy(a, 3, True).wait_recv()
        wsib(a, TWO).start()

    def wend(a):
        wown(a).wait()
        for k in range(4):
            wcopy(a, k).wait_send()
        for dx in range(nx):
            wsib(a, dx, True).wait_recv()
            wsib(a, dx).wait_send()

    def qkv(dx, s):
        b = block(dx, (c + s) % TWO)
        at = pl.ds(pl.multiple_of(b * ntok, ntok), ntok)
        xb = xg[b]
        cs, sn = c_ref[at, :], s_ref[at, :]

        def turned(t):
            return (t * cs + pltpu.roll(t, HEAD // TWO, ONE) * sn)

        k = jnp.dot(xb, wk_ref[...], preferred_element_type=f32)
        for h in range(heads):
            kvb[r, b, h * HEAD:(h + ONE) * HEAD, :] = turned(k[:, h * HEAD:(h + ONE) * HEAD]).T.astype(bf16)
        kvb[r, b, w:, :] = jnp.dot(xb, wv_ref[...], preferred_element_type=f32).astype(bf16)
        q = jnp.dot(xb, wq_ref[...], preferred_element_type=f32)
        for h in range(heads):
            q_s[at, h * HEAD:(h + ONE) * HEAD] = turned(q[:, h * HEAD:(h + ONE) * HEAD]).astype(bf16)
        ycopy(dx, s, 0).start()
        ycopy(dx, s, ONE).start()

    def pass_on(dx, s):
        for k in (0, ONE):
            ycopy(dx, s, k, True).wait_recv()
        for k in (TWO, 3):
            ycopy(dx, s, k).start()

    xcopy(0).start()
    xcopy(ONE).start()
    sib(0).start()
    m_s[...] = jnp.full_like(m_s, -1e30)
    l_s[...] = jnp.zeros_like(l_s)
    acc_s[...] = jnp.zeros_like(acc_s)
    order = ((0, 0), (0, ONE), (nx - ONE, 0), (ONE, 0), (nx - ONE, ONE), (ONE, ONE), (TWO, 0), (TWO, ONE))
    dxs = sum(o[0] << (TWO * i) for i, o in enumerate(order))
    other = sum(o[ONE] << i for i, o in enumerate(order))

    def chunk(n, _):
        @pl.when(n == ONE)
        def _():
            sib(0, True).wait_recv()

        @pl.when(n == TWO)
        def _():
            xcopy(0, True).wait_recv()
            xcopy(TWO).start()
            sib(nx - ONE).start()
            xcopy(ONE, True).wait_recv()
            xcopy(TWO + ONE).start()
            sib(ONE).start()
            wstart(0)
            wstart(ONE)

        for i, dx in ((4, nx - ONE), (5, ONE), (7, TWO)):
            @pl.when(n == i)
            def _():
                sib(dx, True).wait_recv()

        @pl.when(n == 6)
        def _():
            for s in (0, ONE):
                pass_on(0, s)
            xcopy(TWO, True).wait_recv()
            xcopy(TWO + ONE, True).wait_recv()
            sib(TWO).start()

        qkv((dxs >> (TWO * n)) & 3, (other >> n) & ONE)
        return 0

    lax.fori_loop(0, nch, chunk, 0)

    def attend(h, qb, rank, kb, chunks, diag):
        rows = pl.ds(pl.multiple_of(qb * ntok, ntok), ntok)
        cols = slice(h * HEAD, (h + ONE) * HEAD)
        q = q_s[rows, cols]
        sc = []
        for j in range(chunks):
            t = jnp.dot(q, kvb[rank, kb + j, cols, :], preferred_element_type=f32)
            if diag and j == chunks - ONE:
                t = jnp.where(lax.broadcasted_iota(jnp.int32, t.shape, ONE) <= lax.broadcasted_iota(jnp.int32, t.shape, 0), t, -1e30)
            sc.append(t)
        m_old = m_s[h, rows, :]
        top = sc[0]
        for t in sc[ONE:]:
            top = jnp.maximum(top, t)
        m_new = jnp.maximum(m_old, jnp.max(top, axis=ONE, keepdims=True))
        alpha = jnp.exp2((m_old - m_new) * cexp)
        level = jnp.concatenate([m_new] * (ntok // HEAD), axis=ONE)
        ps = [jnp.exp2((t - level) * cexp) for t in sc]
        tot = ps[0]
        for p in ps[ONE:]:
            tot = tot + p
        pv = None
        for j, p in enumerate(ps):
            t = jnp.dot(p.astype(bf16), kvb[rank, kb + j, w:, cols], preferred_element_type=f32)
            pv = t if pv is None else pv + t
        l_s[h, rows, :] = alpha * l_s[h, rows, :] + sum(tot[:, n:n + HEAD] for n in range(0, ntok, HEAD))
        acc_s[h, rows, :] = alpha * acc_s[h, rows, :] + pv
        m_s[h, rows, :] = m_new

    per = nch // TWO

    def own_diag(second, _):
        base = second * per
        for i in range(per):
            for h in range(heads):
                attend(h, base + i, r, base, i + ONE, True)
        return 0

    lax.fori_loop(0, TWO, own_diag, 0)
    def ranks(k, _):
        @pl.when(k == 0)
        def _():
            for dx in (nx - ONE, ONE):
                for s in (0, ONE):
                    pass_on(dx, s)

        @pl.when(k == ONE)
        def _():
            for s in (0, ONE):
                pass_on(TWO, s)
            wpass(0)

        @pl.when(k == TWO)
        def _():
            wlast(0)

        @pl.when(k == ncp - ONE)
        def _():
            wpass(ONE)
            for dx in range(nx):
                for s in (0, ONE):
                    for n in (TWO, TWO + ONE):
                        ycopy(dx, s, n, True).wait_recv()

        dy = jnp.where(k == TWO, ncp - ONE, jnp.where(k == ncp - ONE, TWO, k))
        rank = (r + dy) % ncp
        low = jnp.where(rank < r, 0, per)

        def go(i, _):
            turn = i // per
            for h in range(heads):
                attend(h, jnp.where(turn == 0, per, low) + i % per, rank, turn * low, per, False)
            return 0

        lax.fori_loop(0, jnp.where(k == 0, per, TWO * per), go, 0)
        return 0

    lax.fori_loop(0, ncp, ranks, 0)
    wlast(ONE)
    for h in range(heads):
        o_ref[:, h * HEAD:(h + ONE) * HEAD] = (acc_s[h] / jnp.sum(l_s[h], axis=ONE, keepdims=True)).astype(bf16)

    wend(0)
    wend(ONE)
    for k in range(4):
        xcopy(k).wait_send()
    for dx in range(nx):
        sib(dx).wait_send()
        for s in (0, ONE):
            for k in range(4):
                ycopy(dx, s, k).wait_send()


def attention(x, g, wq, wk, wv, cos, sin, wo, ws2, ncp, ntp):
    ntok, dm = x.shape
    w = wq.shape[ONE]
    heads = w // HEAD
    n = ntok * ntp
    vm = pl.BlockSpec(memory_space=pltpu.VMEM)
    any_ = pl.BlockSpec(memory_space=pl.ANY)
    dma = pltpu.SemaphoreType.DMA
    return pl.pallas_call(
        attn_kernel,
        in_specs=[vm] * 9,
        out_specs=[vm, any_, any_],
        out_shape=[jax.ShapeDtypeStruct((n, w), bf16), jax.ShapeDtypeStruct((ntp,) + wo.shape, bf16),
                   jax.ShapeDtypeStruct((ntp,) + ws2.shape, bf16)],
        scratch_shapes=[pltpu.VMEM((ntp, ntok, dm), bf16), pltpu.VMEM((n, w), bf16), pltpu.VMEM((ncp, ntp, TWO * w, ntok), bf16),
                        pltpu.VMEM((heads, n, HEAD), f32), pltpu.VMEM((heads, n, HEAD), f32), pltpu.VMEM((heads, n, HEAD), f32),
                        dma((4,)), dma((4,)), dma((ntp // TWO,)), dma((ntp // TWO,)), dma((4 * ntp,)), dma((4 * ntp,)),
                        dma((TWO, 4)), dma((TWO, 4)), dma((TWO, ntp // TWO)), dma((TWO, ntp // TWO)), dma((TWO,))],
        compiler_params=pltpu.CompilerParams(collective_id=ONE, has_side_effects=True, vmem_limit_bytes=60 * TWO**20),
        cost_estimate=pl.CostEstimate(flops=6 * n * dm * w + TWO * n * n * ncp * w, bytes_accessed=16 * n * dm, transcendentals=0),
    )(x, g.reshape(ONE, dm), wq, wk, wv, cos, sin, wo, ws2)


ORDER = [(0, 0), (ONE, 0), (3, 0), (0, ONE), (0, 3), (TWO, 0), (0, TWO), (ONE, ONE),
         (ONE, 3), (3, ONE), (3, 3), (TWO, ONE), (TWO, 3), (ONE, TWO), (3, TWO), (TWO, TWO)]
DIST = [0, ONE, TWO, ONE]


def packed(values):
    return [sum(v << (TWO * i) for i, v in enumerate(values[k:k + 8])) for k in (0, 8)]


DX, DY = packed([o[0] for o in ORDER]), packed([o[ONE] for o in ORDER])


def look(table, j):
    a, b = table
    return ((a + (j // 8) * (b - a)) >> (TWO * (j % 8))) & 3


def gather_copies(rows):
    h, q = rows // TWO, rows // 4
    out = []
    for flip in (False, True):
        base = h if flip else 0
        fw = (lambda a, b: (b, a)) if flip else (lambda a, b: (a, b))

        def add(rank, blk, lo, n, step):
            out.append((rank, fw(*blk), base + lo, n, fw(*step)))

        add(0, (0, 0), 0, h, (ONE, 0))
        add(0, (0, 0), 0, h, (3, 0))
        add(ONE, (3, 0), 0, q, (ONE, 0))
        add(ONE, (ONE, 0), q, q, (3, 0))
        for b in (3, ONE, 0, TWO):
            add(TWO, (b, 0), 0, h, (0, ONE))
            add(TWO, (b, 0), 0, h, (0, 3))
            add(3, (b, 3), 0, q, (0, ONE))
            add(3, (b, ONE), q, q, (0, 3))
    out.sort(key=lambda t: t[0])
    return [t[ONE:] for t in out]


def dist(b):
    return DIST[b[0]] + DIST[b[ONE]]


def moe_kernel(nx, ny, cap, groups, t_ref, idx_ref, code_ref, gate_ref, w1g_ref, w1u_ref, w2_ref,
               ws1_ref, ws2_ref, acc_ref, tg_ref, rz_ref, ru_ref, md_ref,
               vg, vu, vd, xin, act, zb, tb, zin, ia, mc_ref,
               wsem, tsem, zsem, lsem, ag_s, ag_r, dd_s, dd_r, rt_s, rt_r, ix_s, ix_r,
               us_s, us_r, ssem, l1_s, l1_r, l2_s, l2_r):
    ntok, dm = t_ref.shape
    ff = w1g_ref.shape[TWO]
    y = lax.axis_index("cp")
    tp = lax.axis_index("tp")
    x, c = tp // TWO, tp % TWO
    nchip = nx * ny
    per = nchip // groups
    homes = TWO * per

    def dev(dx, dy, core):
        return {"cp": (y + dy) % ny, "tp": ((x + dx) % nx) * TWO + core}

    def flat(dx, dy, core):
        return ((y + dy) % ny) * (TWO * nx) + ((x + dx) % nx) * TWO + core

    def weights(l):
        return [pltpu.make_async_copy(a.at[l, pl.ds(k * (a.shape[ONE] // 4), a.shape[ONE] // 4), :],
                                      b.at[l, pl.ds(k * (a.shape[ONE] // 4), a.shape[ONE] // 4), :], wsem.at[l, n, k])
                for n, (a, b) in enumerate(((w1g_ref, vg), (w1u_ref, vu), (w2_ref, vd))) for k in range(4)]

    own = pltpu.make_async_copy(t_ref, tg_ref.at[flat(0, 0, c)], lsem.at[0])

    ia[flat(0, 0, c)] = idx_ref[...]
    barrier = pltpu.get_barrier_semaphore()

    def greet(k, _):
        other = (y * TWO * nx + tp + k) % (TWO * nchip)
        pl.semaphore_signal(barrier, inc=ONE, device_id={"cp": other // (TWO * nx), "tp": other % (TWO * nx)}, device_id_type=MESH)
        return 0

    lax.fori_loop(ONE, TWO * nchip, greet, 0)
    pl.semaphore_wait(barrier, TWO * nchip - ONE)

    copies = gather_copies(ntok)

    def ici(k):
        blk, lo, n, step = copies[k]
        here = tg_ref.at[flat(blk[0], blk[ONE], c), pl.ds(lo, n), :]
        src = t_ref.at[pl.ds(lo, n), :] if blk == (0, 0) else here
        return pltpu.make_async_remote_copy(src_ref=src, dst_ref=here, send_sem=ag_s.at[k], recv_sem=ag_r.at[k],
                                            device_id=dev(step[0], step[ONE], c), device_id_type=MESH)

    def ici_in(k):
        blk, lo, n, step = copies[k]
        here = tg_ref.at[flat(blk[0] - step[0] + nx, blk[ONE] - step[ONE] + ny, c), pl.ds(lo, n), :]
        return pltpu.make_async_remote_copy(src_ref=here, dst_ref=here, send_sem=ag_s.at[k], recv_sem=ag_r.at[k],
                                            device_id=dev(nx - step[0], ny - step[ONE], c), device_id_type=MESH)

    def d2d(j, core):
        blk = ORDER[j]
        here = tg_ref.at[flat(blk[0], blk[ONE], core)]
        src = t_ref if (j == 0) else here
        return pltpu.make_async_remote_copy(src_ref=src, dst_ref=here, send_sem=dd_s.at[j], recv_sem=dd_r.at[j],
                                            device_id=dev(0, 0, ONE - c), device_id_type=MESH)

    def d2d_in(j):
        blk = ORDER[j]
        here = tg_ref.at[flat(blk[0], blk[ONE], ONE - c)]
        return pltpu.make_async_remote_copy(src_ref=here, dst_ref=here, send_sem=dd_s.at[j], recv_sem=dd_r.at[j],
                                            device_id=dev(0, 0, ONE - c), device_id_type=MESH)

    def round_(w):
        h = ntok // TWO
        if w == 0:
            for k, cp in enumerate(copies):
                if cp[0] == (0, 0):
                    ici(k).start()
            d2d(0, c).start()
            return
        left = {}
        into = [(k, ((cp[0][0] - cp[3][0]) % nx, (cp[0][ONE] - cp[3][ONE]) % ny), cp) for k, cp in enumerate(copies) if dist(cp[0]) == w - ONE]
        for k, blk, cp in into:
            part = (blk, cp[ONE] // h)
            left[part] = left.get(part, 0) + cp[TWO]
        done = {}
        for k, blk, cp in into:
            ici_in(k).wait_recv()
            part = (blk, cp[ONE] // h)
            left[part] -= cp[TWO]
            if left[part] == 0:
                for n, out in enumerate(copies):
                    if out[0] == blk and out[ONE] // h == part[ONE]:
                        ici(n).start()
                done[blk] = done.get(blk, 0) + ONE
                if done[blk] == TWO:
                    d2d(ORDER.index(blk), c).start()

    def siblings(w):
        for j, b in enumerate(ORDER):
            if dist(b) == w:
                d2d_in(j).wait_recv()

    def choices(j, s, incoming=False):
        core = c if s == 0 else ONE - c
        dx, dy = look(DX, j), look(DY, j)
        ref = ia.at[flat(nx - dx, ny - dy, core) if incoming else flat(0, 0, c)]
        return pltpu.make_async_remote_copy(src_ref=ref, dst_ref=ref, send_sem=ix_s.at[TWO * j + s], recv_sem=ix_r.at[TWO * j + s],
                                            device_id=dev(nx - dx, ny - dy, core) if incoming else dev(dx, dy, core),
                                            device_id_type=MESH)

    def each_other(do):
        def go(j, _):
            @pl.when(j > 0)
            def _():
                do(j, 0)

            do(j, ONE)
            return 0

        lax.fori_loop(0, nchip, go, 0)

    each_other(lambda j, s: choices(j, s).start())
    round_(0)
    own.start()
    for l in range(TWO):
        for p in weights(l):
            p.start()

    def back(j, s, slot):
        core = c if s == 0 else ONE - c
        return pltpu.make_async_remote_copy(src_ref=zb.at[slot], dst_ref=rz_ref.at[slot], send_sem=rt_s.at[slot],
                                            recv_sem=rt_r.at[slot],
                                            device_id=dev(look(DX, j), look(DY, j), core), device_id_type=MESH)

    straight = sum(0 in o for o in ORDER)

    def cols(half):
        return pl.ds(half * (dm // TWO), dm // TWO)

    def leg1(j, half, incoming=False):
        dx, dy = ORDER[j]
        step = (0, dy) if half else (dx, 0)
        if incoming:
            step = (nx - step[0], ny - step[ONE])
        return pltpu.make_async_remote_copy(src_ref=zb.at[pl.ds(TWO * j, TWO), :, cols(half)], dst_ref=md_ref.at[j - straight, half],
                                            send_sem=l1_s.at[j - straight, half], recv_sem=l1_r.at[j - straight, half],
                                            device_id=dev(step[0], step[ONE], c), device_id_type=MESH)

    def leg2(j, s, half):
        step = (look(DX, j), 0) if half else (0, look(DY, j))
        return pltpu.make_async_remote_copy(src_ref=md_ref.at[j - straight, half, s], dst_ref=rz_ref.at[TWO * j + s, :, cols(half)],
                                            send_sem=l2_s.at[j - straight, s, half], recv_sem=l2_r.at[j - straight, s, half],
                                            device_id=dev(step[0], step[ONE], ONE - c if s else c), device_id_type=MESH)

    def leg2_in(j, s, half):
        step = (look(DX, j), 0) if half else (0, look(DY, j))
        return pltpu.make_async_remote_copy(src_ref=md_ref.at[j - straight, half, s], dst_ref=rz_ref.at[TWO * j + s, :, cols(half)],
                                            send_sem=l2_s.at[j - straight, s, half], recv_sem=l2_r.at[j - straight, s, half],
                                            device_id=dev(nx - step[0], ny - step[ONE], ONE - c if s else c), device_id_type=MESH)

    def forward(j):
        for half in range(TWO):
            leg1(j, half, True).wait_recv()
            for s in range(TWO):
                leg2(j, s, half).start()

    wide = ws1_ref.shape[ONE] // TWO
    deep = ws2_ref.shape[ONE]

    def ublock(i):
        return xin.at[i // nx, pl.ds(0, ntok), pl.ds((i % nx) * wide, wide)]

    def ucopy(i, incoming=False):
        dx, core = i // TWO, c if i % TWO == 0 else ONE - c
        return pltpu.make_async_remote_copy(src_ref=ublock(i), dst_ref=ru_ref.at[i], send_sem=us_s.at[i], recv_sem=us_r.at[i],
                                            device_id=dev(nx - dx if incoming else dx, 0, core), device_id_type=MESH)

    def uown():
        return pltpu.make_async_copy(ublock(0), ru_ref.at[0], us_s.at[0])

    def ws2_load(i):
        j = ((x + nx - i // TWO) % nx) * TWO + (c if i % TWO == 0 else ONE - c)
        return pltpu.make_async_copy(ws2_ref.at[j], vd.at[i // nx, pl.ds((i % nx) * deep, deep), :], ssem.at[ONE + i])

    def shared_up():
        first = pltpu.make_async_copy(ws1_ref, vg.at[0, :, pl.ds(0, TWO * wide)], ssem.at[0])
        first.start()

        def rows_of(i):
            d = flat(i // TWO, 0, c if i % TWO == 0 else ONE - c)
            return pltpu.make_async_copy(tg_ref.at[d], tb.at[i % DEPTH], tsem.at[i % DEPTH])

        for i in range(DEPTH - ONE):
            rows_of(i).start()
        for i in range(TWO * nx):
            ws2_load(i).start()
        first.wait()
        for i in range(TWO * nx):
            rows_of(i).wait()
            if i + DEPTH - ONE < TWO * nx:
                rows_of(i + DEPTH - ONE).start()
            a = jnp.dot(tb[i % DEPTH], vg[0, :, :wide], preferred_element_type=f32)
            b = jnp.dot(tb[i % DEPTH], vg[0, :, wide:TWO * wide], preferred_element_type=f32)
            xin[i // nx, :ntok, (i % nx) * wide:(i % nx + ONE) * wide] = (a * jax.nn.sigmoid(a) * b).astype(bf16)
        uown().start()
        for i in range(ONE, TWO * nx):
            ucopy(i).start()

    def shared_down():
        uown().wait()
        pulls = []
        for i in range(TWO * nx):
            if i:
                ucopy(i, True).wait_recv()
            p = pltpu.make_async_copy(ru_ref.at[i], tb.at[i // nx, :, pl.ds((i % nx) * wide, wide)], ssem.at[9 + i])
            p.start()
            pulls.append(p)
        for i in range(TWO * nx):
            ws2_load(i).wait()
            pulls[i].wait()

        def col(n, _):
            at = pl.ds(pl.multiple_of(n * 256, 256), 256)
            tot = acc_ref[:, at]
            for i in range(TWO * nx):
                tot = tot + jnp.dot(tb[i // nx, :, (i % nx) * wide:(i % nx) * wide + deep],
                                    vd[i // nx, (i % nx) * deep:(i % nx + ONE) * deep, at], preferred_element_type=f32)
            acc_ref[:, at] = tot
            return 0

        lax.fori_loop(0, dm // 256, col, 0)

    def work(g, _):
        for w in range(ONE, 5):
            @pl.when(g == w - ONE)
            def _():
                round_(w)
                if w == ONE:
                    siblings(0)
                siblings(w)
                if w == ONE:
                    own.wait()
                    each_other(lambda j, s: choices(j, s, True).wait_recv())
                    upto = (lax.broadcasted_iota(jnp.int32, (ntok, ntok), 0)
                            <= lax.broadcasted_iota(jnp.int32, (ntok, ntok), ONE)).astype(f32).astype(bf16)
                    for l in range(TWO):
                        e = (y * TWO * nx + tp) * TWO + l
                        hit = jnp.zeros((TWO * nchip, ntok), jnp.bool_)
                        for k in range(code_ref.shape[ONE]):
                            hit = hit | (ia[:, k, :] == e)
                        hit = hit.astype(f32)
                        cum = jnp.dot(hit.astype(bf16), upto, preferred_element_type=f32)
                        mc_ref[l] = (hit * cum).astype(jnp.int32)

        @pl.when(g == groups - ONE)
        def _():
            forward(straight)

        def fetch(i):
            j = g * per + i // TWO
            core = c if i % TWO == 0 else ONE - c
            d = flat(look(DX, j), look(DY, j), core)
            return d, pltpu.make_async_copy(tg_ref.at[d], tb.at[i % DEPTH], tsem.at[i % DEPTH])

        for i in range(DEPTH - ONE):
            fetch(i)[ONE].start()
        for i in range(homes):
            d, cp = fetch(i)
            cp.wait()
            if i + DEPTH - ONE < homes:
                fetch(i + DEPTH - ONE)[ONE].start()
            rows = lax.broadcasted_iota(jnp.int32, (TWO * cap, ntok), 0)
            rank = jnp.where(rows < cap, mc_ref[0, pl.ds(d, ONE), :], mc_ref[ONE, pl.ds(d, ONE), :])
            sel = (rank == jnp.where(rows < cap, rows, rows - cap) + ONE).astype(f32).astype(bf16)
            def pick(n, _):
                at = pl.ds(pl.multiple_of(n * 1024, 1024), 1024)
                got = jnp.dot(sel, tb[i % DEPTH, :, at], preferred_element_type=f32)
                xin[0, i * cap:(i + ONE) * cap, at] = got[:cap].astype(bf16)
                xin[ONE, i * cap:(i + ONE) * cap, at] = got[cap:].astype(bf16)
                return 0

            lax.fori_loop(0, dm // 1024, pick, 0)

        def expert(l, _):
            @pl.when(g == 0)
            def _():
                for p in weights(l):
                    p.wait()

            def up(at, n):
                a = jnp.dot(xin[l], vg[l, :, pl.ds(at, n)], preferred_element_type=f32)
                b = jnp.dot(xin[l], vu[l, :, pl.ds(at, n)], preferred_element_type=f32)
                act[:, pl.ds(at, n)] = (a * jax.nn.sigmoid(a) * b).astype(bf16)

            whole = ff // 256
            lax.fori_loop(0, whole, lambda n, _: (up(pl.multiple_of(n * 256, 256), 256), 0)[ONE], 0)
            if ff % 256:
                up(whole * 256, ff % 256)

            def down(n, _):
                at = pl.multiple_of(n * 256, 256)
                z = jnp.dot(act[...], vd[l, :, pl.ds(at, 256)], preferred_element_type=f32)
                for k in range(TWO):
                    @pl.when(l == k)
                    def _():
                        for i in range(homes):
                            zb[g * homes + i, k * cap:(k + ONE) * cap, pl.ds(at, 256)] = z[i * cap:(i + ONE) * cap].astype(bf16)
                return 0

            lax.fori_loop(0, dm // 256, down, 0)
            return 0

        lax.fori_loop(0, TWO, expert, 0)

        @pl.when(g == 0)
        def _():
            pltpu.make_async_copy(zb.at[0], rz_ref.at[0], lsem.at[ONE]).start()

        for k in range(groups):
            @pl.when(g == k)
            def _():
                if k == groups - ONE:
                    shared_up()
                mine = range(k * per, (k + ONE) * per)
                for j in mine:
                    if j >= straight:
                        leg1(j, 0).start()
                        leg1(j, ONE).start()
                for s in range(TWO):
                    for j in mine:
                        if j < straight and j + s:
                            back(j, s, TWO * j + s).start()

        return 0

    lax.fori_loop(0, groups, work, 0)
    for j in range(straight + ONE, nchip):
        forward(j)

    acc_ref[...] = jnp.zeros_like(acc_ref)

    def arrived(j, s, slot):
        core = c if s == 0 else ONE - c
        return pltpu.make_async_remote_copy(src_ref=zb.at[slot], dst_ref=rz_ref.at[slot], send_sem=rt_s.at[slot],
                                            recv_sem=rt_r.at[slot],
                                            device_id=dev(nx - look(DX, j), ny - look(DY, j), core), device_id_type=MESH)

    def combine(j, _):
        @pl.when(j == nchip - per)
        def _():
            shared_down()

        @pl.when(j == 0)
        def _():
            pltpu.make_async_copy(zb.at[0], rz_ref.at[0], lsem.at[ONE]).wait()

        @pl.when((j > 0) & (j < straight))
        def _():
            arrived(j, 0, TWO * j).wait_recv()

        @pl.when(j < straight)
        def _():
            arrived(j, ONE, TWO * j + ONE).wait_recv()

        @pl.when(j >= straight)
        def _():
            for s in range(TWO):
                for half in range(TWO):
                    leg2_in(j, s, half).wait_recv()

        pulls = [pltpu.make_async_copy(rz_ref.at[TWO * j + s], zin.at[pl.ds(s * TWO * cap, TWO * cap), :], zsem.at[s]) for s in range(TWO)]
        for p in pulls:
            p.start()
        base = [flat(nx - look(DX, j), ny - look(DY, j), core) * (TWO * cap) for core in (c, ONE - c)]
        lane = lax.broadcasted_iota(jnp.int32, (ntok, 4 * cap), ONE)
        want = jnp.where(lane < TWO * cap, base[0] + lane, base[ONE] + lane - TWO * cap)
        g = jnp.zeros((ntok, 4 * cap), f32)
        for k in range(code_ref.shape[ONE]):
            g = g + jnp.where(code_ref[:, k:k + ONE] == want, gate_ref[:, k:k + ONE], 0.0)
        g1 = g.astype(bf16)
        rest = g - g1.astype(f32)
        g2 = rest.astype(bf16)
        g3 = (rest - g2.astype(f32)).astype(bf16)
        for p in pulls:
            p.wait()

        def col(n, _):
            at = pl.ds(pl.multiple_of(n * 512, 512), 512)
            z = zin[:, at]
            acc_ref[:, at] += (jnp.dot(g1, z, preferred_element_type=f32)
                               + (jnp.dot(g2, z, preferred_element_type=f32) + jnp.dot(g3, z, preferred_element_type=f32)))
            return 0

        lax.fori_loop(0, dm // 512, col, 0)
        return 0

    lax.fori_loop(0, nchip, combine, 0)

    for k in range(len(copies)):
        ici(k).wait_send()
    for j in range(nchip):
        d2d(j, c).wait_send()

    each_other(lambda j, s: choices(j, s).wait_send())
    for j in range(nchip):
        for s in range(TWO):
            if j >= straight:
                leg1(j, s).wait_send()
                for half in range(TWO):
                    leg2(j, s, half).wait_send()
            elif j + s:
                back(j, s, TWO * j + s).wait_send()
    for i in range(ONE, TWO * nx):
        ucopy(i).wait_send()


def moe(t, idx, code, gates, w1g, w1u, w2, ws1, ws2, nx, ny, cap):
    ntok, dm = t.shape
    nle, _, ff = w1g.shape
    ndev = TWO * nx * ny
    groups = 4
    rows = ndev // groups * cap
    any_ = pl.BlockSpec(memory_space=pl.ANY)
    vm = pl.BlockSpec(memory_space=pltpu.VMEM)
    ncopy = len(gather_copies(ntok))
    turns = sum(0 not in o for o in ORDER)
    dma = pltpu.SemaphoreType.DMA
    return pl.pallas_call(
        functools.partial(moe_kernel, nx, ny, cap, groups),
        in_specs=[vm, vm, vm, vm] + [any_] * 5,
        out_specs=[vm] + [any_] * 4,
        out_shape=[jax.ShapeDtypeStruct((ntok, dm), f32),
                   jax.ShapeDtypeStruct((ndev, ntok, dm), bf16),
                   jax.ShapeDtypeStruct((ndev, nle * cap, dm), bf16),
                   jax.ShapeDtypeStruct((TWO * nx, ntok, ws1.shape[ONE] // TWO), bf16),
                   jax.ShapeDtypeStruct((turns, TWO, TWO, nle * cap, dm // TWO), bf16)],
        scratch_shapes=[pltpu.VMEM((nle, dm, ff), bf16), pltpu.VMEM((nle, dm, ff), bf16), pltpu.VMEM((nle, ff, dm), bf16),
                        pltpu.VMEM((nle, rows, dm), bf16), pltpu.VMEM((rows, ff), bf16),
                        pltpu.VMEM((ndev, nle * cap, dm), bf16), pltpu.VMEM((DEPTH, ntok, dm), bf16),
                        pltpu.VMEM((TWO * nle * cap, dm), bf16), pltpu.VMEM((ndev,) + idx.shape, jnp.int32),
                        pltpu.VMEM((nle, ndev, ntok), jnp.int32),
                        dma((TWO, 3, 4)), dma((DEPTH,)), dma((TWO,)), dma((TWO,)), dma((ncopy,)), dma((ncopy,)),
                        dma((nx * ny,)), dma((nx * ny,)), dma((ndev,)), dma((ndev,)), dma((ndev,)), dma((ndev,)),
                        dma((TWO * nx,)), dma((TWO * nx,)), dma((17,)), dma((turns, TWO)), dma((turns, TWO)),
                        dma((turns, TWO, TWO)), dma((turns, TWO, TWO))],
        compiler_params=pltpu.CompilerParams(collective_id=0, has_side_effects=True, vmem_limit_bytes=VMEM_MAX),
        cost_estimate=pl.CostEstimate(flops=6 * ndev * nle * cap * dm * ff, bytes_accessed=10 * nle * dm * ff, transcendentals=0),
    )(t, idx, code, gates, w1g, w1u, w2, ws1, ws2)


def solution(mesh):
    ncp = mesh.shape["cp"]
    ntp = mesh.shape["tp"]
    ndev = ncp * ntp
    rows = P(("dp", "cp", "tp"), None)
    cols = P(None, "tp")
    wrows = P("tp", None)
    rep = P(None)
    exps = P(("cp", "tp"), None, None)

    def layer(x, g_attn, wq, wk, wv, wo, g_mlp, idx, gates, w1g, w1u, w2, ws1g, ws1u, ws2):
        r = lax.axis_index("cp")
        me = r * ntp + lax.axis_index("tp")
        ntok, dm = x.shape
        seq = ntok * ndev
        nloc = seq // ncp
        nle = w1g.shape[0]
        num_e = nle * ndev
        top = idx.shape[ONE]
        cap = -(-top * (TWO * ntok // num_e + ONE) // 8) * 8

        upto = (jnp.arange(ntok)[:, None] <= jnp.arange(ntok)[None, :]).astype(bf16)
        named = idx[:, :, None] == jnp.arange(num_e)[None, None, :]
        before = lax.dot_general(upto, jnp.any(named, axis=ONE).astype(bf16), (((0,), (0,)), ((), ())), preferred_element_type=f32) - 1.0
        rank = jnp.sum(jnp.where(named, before[:, None, :], 0.0), axis=-ONE).astype(jnp.int32)
        code = idx * cap + rank

        half = HEAD // TWO
        pos = layout_pos(r * nloc + jnp.arange(nloc), ncp, seq)
        freq = ROPE_BASE ** (-jnp.arange(half, dtype=f32) / half)
        ang = pos.astype(f32)[:, None] * freq[None, :]
        cs, sn = jnp.cos(ang), jnp.sin(ang)
        o, wo_all, ws2_all = attention(x, g_attn, wq, wk, wv, jnp.concatenate([cs, cs], ONE), jnp.concatenate([-sn, sn], ONE), wo, ws2, ncp, ntp)
        o = lax.all_to_all(o, "tp", 0, ONE, tiled=True)
        attn = jnp.dot(o, wo_all.reshape(-ONE, dm), preferred_element_type=f32)
        h = (x.astype(f32) + attn).astype(bf16)
        t = rms_norm(h, g_mlp)

        idx_t = jnp.pad(idx.T, ((0, 8 - top), (0, 0)), constant_values=-ONE)
        pad = ((0, 0), (0, -ws1g.shape[ONE] % 128))
        ws1 = jnp.concatenate([jnp.pad(ws1g, pad), jnp.pad(ws1u, pad)], axis=ONE)
        added = moe(t, idx_t, code, gates, w1g, w1u, w2, ws1, ws2_all, ntp // TWO, ncp, cap)[0]
        return (h.astype(f32) + added).astype(bf16)

    return jax.shard_map(layer, mesh=mesh,
                         in_specs=(rows, rep, cols, cols, cols, wrows, rep, rows, rows, exps, exps, exps, cols, cols, wrows),
                         out_specs=rows, check_vma=False)
```
